32 devices in a mesh: batch: 1 (over z), cy: 4 (over y), cx: 8 (over x, core).
Axes of the slice: x: 4, y: 4, z: 1, core: 2. Of those that a mesh axis runs over, the one named last changes fastest.
The devices are a block of a 4x4x8 slice.
Arguments:
- q_seq: bfloat16 [4096, 32, 64], P(('batch', 'cx', 'cy'))
- k_seq: bfloat16 [4096, 8, 64], P(('batch', 'cx', 'cy'))
- v_seq: bfloat16 [4096, 8, 64], P(('batch', 'cx', 'cy'))
Outputs:
- output: bfloat16 [4096, 32, 64], P(('batch', 'cx', 'cy'))
All inputs are finite; a program needn't handle non-finite values.
Results may differ from the reference program's by a relative error of at most 0.00508428.
Values are sent between devices in bfloat16 or wider.
A program may use at most 768 MiB of HBM per device.

```python
import math
import jax
import jax.numpy as jnp
from jax import lax

SEQ = 4096
HEADS = 32
KV_HEADS = 8
HEAD = 64
Q_BLOCK = 32

GROUP_HEADS = HEADS // KV_HEADS
SCORE_STD = math.sqrt(max(1.0, math.log(SEQ / 64.0)))


def setup_inputs(seed: int = 0, part: int = 0) -> dict:
    base_key = jax.random.fold_in(jax.random.key(seed), part)
    key_q, key_k, key_v = jax.random.split(base_key, 3)
    in_scale = math.sqrt(SCORE_STD)
    q_seq = jax.random.normal(key_q, (SEQ, HEADS, HEAD), jnp.float32) * in_scale
    k_seq = jax.random.normal(key_k, (SEQ, KV_HEADS, HEAD), jnp.float32) * in_scale
    v_seq = jax.random.normal(key_v, (SEQ, KV_HEADS, HEAD), jnp.float32) * 2.0
    return {"q_seq": q_seq.astype(jnp.bfloat16), "k_seq": k_seq.astype(jnp.bfloat16), "v_seq": v_seq.astype(jnp.bfloat16)}


def reference(q_seq, k_seq, v_seq):
    score_scale = 1.0 / math.sqrt(HEAD)
    keys_wide = k_seq.astype(jnp.float32)
    vals_wide = v_seq.astype(jnp.float32)
    q_blocks = q_seq.reshape(SEQ // Q_BLOCK, Q_BLOCK, KV_HEADS, GROUP_HEADS, HEAD)

    def attend_block(q_part):
        scores = jnp.einsum("qkgd,skd->kgqs", q_part.astype(jnp.float32), keys_wide) * score_scale
        row_max = jnp.max(scores, axis=-1, keepdims=True)
        prob_all = jnp.exp(scores - row_max)
        row_sum = jnp.sum(prob_all, axis=-1)
        weighted = jnp.einsum("kgqs,skd->qkgd", prob_all.astype(jnp.bfloat16).astype(jnp.float32), vals_wide)
        result = weighted / jnp.transpose(row_sum, (2, 0, 1))[..., None]
        return result.astype(jnp.bfloat16)

    out_blocks = lax.map(attend_block, q_blocks)
    return out_blocks.reshape(SEQ, HEADS, HEAD)
```

```python
import functools
import math

import jax
import jax.numpy as jnp
from jax import lax
from jax.experimental import pallas as pl
from jax.experimental.pallas import tpu as pltpu
from jax.sharding import PartitionSpec as P

F32 = jnp.float32
BF16 = jnp.bfloat16
MESH = pl.DeviceIdType.MESH

TILE = 256
MEMBERS = 8
BLOCKS = 4
EARLY = 2


def flip(value):
    return value + 1 - 2 * lax.rem(value, 2)


def attend_kernel(
    size_x, size_y, scale,
    q_ref, k_ref, v_ref, out_ref,
    q_got, kv_got, keys, q_limbs, scores, probs, block_max, row_max, row_sum, rescale, acc, out_send,
    kv_sent, kv_here, q_sent, q_here, fwd_sent, fwd_here, out_sent, out_here,
):
    head_dim, tokens = k_ref.shape[1:]
    group = q_ref.shape[0] // k_ref.shape[0]
    tiles = group * tokens // TILE
    per_tile = TILE // tokens
    span = MEMBERS * tokens
    steps = MEMBERS * BLOCKS
    turn = MEMBERS * EARLY
    late = BLOCKS - EARLY

    ix = lax.axis_index("cx")
    iy = lax.axis_index("cy")
    chips_x = size_x // 2
    chip_x, core = ix // 2, lax.rem(ix, 2)
    half_x, half_y = chips_x // 2, size_y // 2

    def head_of(x, y, c):
        px = lax.rem(x + x // half_x, 2)
        py = lax.rem(y + y // half_y, 2)
        return px * 4 + py * 2 + c

    def member(r):
        x = flip(chip_x) if r // 4 else chip_x
        y = flip(iy) if (r // 2) % 2 else iy
        c = flip(core) if r % 2 else core
        return {"cx": x * 2 + c, "cy": y}, head_of(x, y, c)

    my_head = head_of(chip_x, iy, core)
    mirror_x = {"cx": (chips_x - 1 - chip_x) * 2 + core, "cy": iy}
    mirror_y = {"cx": ix, "cy": size_y - 1 - iy}

    barrier = pltpu.get_barrier_semaphore()
    partners = [member(r)[0] for r in range(1, MEMBERS)] + [mirror_x, mirror_y]
    for who in partners:
        pl.semaphore_signal(barrier, inc=1, device_id=who, device_id_type=MESH)
    pl.semaphore_wait(barrier, len(partners))

    def remote(src, dst, sent, here, who):
        return pltpu.make_async_remote_copy(
            src_ref=src, dst_ref=dst, send_sem=sent, recv_sem=here, device_id=who, device_id_type=MESH
        )

    def send_kv(k_src, v_src, slot, sent, here, who):
        remote(k_src, slot.at[pl.ds(0, head_dim)], sent, here, who).start()
        remote(v_src, slot.at[pl.ds(head_dim, head_dim)], sent, here, who).start()

    def kv_whole(r):
        slot = kv_got.at[0, r]
        return remote(slot, slot, kv_sent.at[r], kv_here.at[r], member(r)[0])

    def q_copy(r):
        who, head = member(r)
        return remote(q_ref.at[pl.ds(head * group, group)], q_got.at[r], q_sent.at[r], q_here.at[r], who)

    def forward(block, r):
        index = (block - 1) * MEMBERS + r
        if block == 3:
            src, who = (kv_got.at[1, r], mirror_y) if r < 4 else (kv_got.at[2, r], mirror_x)
        else:
            src, who = kv_got.at[0, r], mirror_x if block == 1 else mirror_y
        return remote(src, kv_got.at[block, r], fwd_sent.at[index], fwd_here.at[index], who)

    def out_copy(r, head):
        return remote(
            out_send.at[r], out_ref.at[pl.ds(head * group, group)], out_sent.at[r], out_here.at[r], member(r)[0]
        )

    for r in range(1, MEMBERS):
        who, head = member(r)
        send_kv(k_ref.at[head], v_ref.at[head], kv_got.at[0, r], kv_sent.at[r], kv_here.at[r], who)
    for block, who in ((1, mirror_x), (2, mirror_y)):
        index = (block - 1) * MEMBERS
        send_kv(k_ref.at[my_head], v_ref.at[my_head], kv_got.at[block, 0], fwd_sent.at[index], fwd_here.at[index], who)
    for r in range(1, MEMBERS):
        q_copy(r).start()

    def prepare_keys(block, r, columns):
        base = block * span + r * tokens
        keys[pl.ds(base, tokens)] = jnp.transpose(jnp.concatenate([columns, columns], axis=0))

    def prepare_queries(r, read):
        for g in range(group):
            wide = read(g).astype(F32) * scale
            high = wide.astype(BF16)
            rest = wide - high.astype(F32)
            middle = rest.astype(BF16)
            low = (rest - middle.astype(F32)).astype(BF16)
            cols = pl.ds(g % per_tile * tokens, tokens)
            for n, term in enumerate((high, middle, low)):
                q_limbs[r, g // per_tile, pl.ds(n * head_dim, head_dim), cols] = term

    def step_q(i):
        return jnp.where(i < turn, lax.rem(i, MEMBERS), MEMBERS - 1 - (i - turn) // late)

    def step_b(i):
        return jnp.where(i < turn, i // MEMBERS, EARLY + lax.rem(i, late))

    def score(i):
        r, b = step_q(i), step_b(i)
        doubled = keys[pl.ds(pl.multiple_of(b * span, span), span)]
        lhs = jnp.concatenate([doubled, doubled], axis=1)
        for t in range(tiles):
            s = jnp.dot(lhs, q_limbs[r, t], preferred_element_type=F32)
            scores[t] = s
            block_max[t] = jnp.max(s.reshape(span // 8, 8, TILE), axis=0)

    def soften(i):
        r = step_q(i)
        for t in range(tiles):
            old = row_max[r, t]
            new = jnp.maximum(old, jnp.max(block_max[t], axis=0, keepdims=True))
            row_max[r, t] = new
            factor = jnp.exp2(old - new)
            rescale[t] = factor
            p = jnp.exp2(scores[t].reshape(span // 8, 8, TILE) - new[None])
            row_sum[r, t] = row_sum[r, t] * factor + jnp.sum(p, axis=0)
            probs[t] = p.reshape(span, TILE).astype(BF16)

    def weigh(i):
        r, b = step_q(i), step_b(i)
        values = jnp.concatenate([kv_got[b, m, pl.ds(head_dim, head_dim)] for m in range(MEMBERS)], axis=1)
        for t in range(tiles):
            weighted = jnp.dot(values, probs[t], preferred_element_type=F32)
            acc[r, t] = acc[r, t] * rescale[t][0:1] + weighted

    def body(i, carry=0):
        weigh(jnp.maximum(i - 1, 0))
        soften(i)
        score(i + 1)
        return carry

    def run(start, stop):
        if stop > start:
            lax.fori_loop(start, stop, body, 0)

    def finish(r):
        for t in range(tiles):
            inverse = 1.0 / jnp.sum(row_sum[r, t], axis=0, keepdims=True)
            result = (acc[r, t] * inverse).astype(BF16)
            for n in range(per_tile):
                part = result[:, n * tokens:(n + 1) * tokens]
                if r == 0:
                    out_ref[my_head * group + t * per_tile + n] = part
                else:
                    out_send[r, t * per_tile + n] = part

    row_max[...] = jnp.full_like(row_max, -jnp.inf)
    row_sum[...] = jnp.zeros_like(row_sum)
    rescale[...] = jnp.ones_like(rescale)
    acc[...] = jnp.zeros_like(acc)
    probs[...] = jnp.zeros_like(probs)
    q_limbs[:, :, pl.ds(3 * head_dim, TILE - 3 * head_dim)] = jnp.zeros(
        (MEMBERS, tiles, TILE - 3 * head_dim, TILE), BF16
    )
    prepare_queries(0, lambda g: q_ref[my_head * group + g])
    prepare_keys(0, 0, k_ref[my_head])
    kv_got[0, 0, pl.ds(head_dim, head_dim)] = v_ref[my_head]

    for r in range(1, MEMBERS):
        kv_whole(r).wait_recv()
        forward(1, r).start()
        forward(2, r).start()
        prepare_keys(0, r, kv_got[0, r, :head_dim])
    score(0)
    for r in range(1, MEMBERS):
        q_copy(r).wait_recv()
        prepare_queries(r, lambda g: q_got[r, g])
        if r == 3:
            for m in range(4):
                forward(1, m).wait_recv()
                forward(3, m).start()
        if r == 6:
            for m in range(4, MEMBERS):
                forward(2, m).wait_recv()
                forward(3, m).start()
        run(r - 1, r)

    done = MEMBERS - 1
    for block in range(1, BLOCKS):
        first = block * MEMBERS if block <= EARLY else turn + block - EARLY
        run(done, first - 1)
        done = first - 1
        for r in range(MEMBERS):
            if (block, r // 4) not in ((1, 0), (2, 1)):
                forward(block, r).wait_recv()
        for r in range(MEMBERS):
            prepare_keys(block, r, kv_got[block, r, :head_dim])

    for r in range(MEMBERS - 1, 0, -1):
        stop = turn + (MEMBERS - r) * late + 1
        if stop < steps:
            run(done, stop)
            done = stop
        else:
            run(done, steps - 1)
            done = steps - 1
        if r < MEMBERS - 1:
            out_copy(r + 1, my_head).start()
        finish(r)
    assert done == steps - 1
    weigh(steps - 2)
    soften(steps - 1)
    out_copy(1, my_head).start()
    weigh(steps - 1)
    finish(0)

    for r in range(1, MEMBERS):
        out_copy(r, member(r)[1]).wait_recv()
        out_copy(r, my_head).wait_send()
        kv_whole(r).wait_send()
        q_copy(r).wait_send()
    for block in range(1, BLOCKS):
        for r in range(MEMBERS):
            forward(block, r).wait_send()


def solution(mesh):
    size_x = mesh.shape["cx"]
    size_y = mesh.shape["cy"]
    seq_spec = P(("batch", "cx", "cy"), None, None)

    def local_attention(q_local, k_local, v_local):
        tokens, num_heads, head_dim = q_local.shape
        num_kv = k_local.shape[1]
        group = num_heads // num_kv
        tiles = group * tokens // TILE
        span = MEMBERS * tokens
        scale = 1.0 / math.sqrt(head_dim) / math.log(2.0)
        vmem = pl.BlockSpec(memory_space=pltpu.VMEM)
        out_cols = pl.pallas_call(
            functools.partial(attend_kernel, size_x, size_y, scale),
            out_shape=jax.ShapeDtypeStruct((num_heads, head_dim, tokens), BF16),
            in_specs=[vmem] * 3,
            out_specs=vmem,
            scratch_shapes=[
                pltpu.VMEM((MEMBERS, group, head_dim, tokens), BF16),
                pltpu.VMEM((BLOCKS, MEMBERS, 2 * head_dim, tokens), BF16),
                pltpu.VMEM((BLOCKS * span, 2 * head_dim), BF16),
                pltpu.VMEM((MEMBERS, tiles, TILE, TILE), BF16),
                pltpu.VMEM((tiles, span, TILE), F32),
                pltpu.VMEM((tiles, span, TILE), BF16),
                pltpu.VMEM((tiles, 8, TILE), F32),
                pltpu.VMEM((MEMBERS, tiles, 8, TILE), F32),
                pltpu.VMEM((MEMBERS, tiles, 8, TILE), F32),
                pltpu.VMEM((tiles, 8, TILE), F32),
                pltpu.VMEM((MEMBERS, tiles, head_dim, TILE), F32),
                pltpu.VMEM((MEMBERS, group, head_dim, tokens), BF16),
                pltpu.SemaphoreType.DMA((MEMBERS,)),
                pltpu.SemaphoreType.DMA((MEMBERS,)),
                pltpu.SemaphoreType.DMA((MEMBERS,)),
                pltpu.SemaphoreType.DMA((MEMBERS,)),
                pltpu.SemaphoreType.DMA(((BLOCKS - 1) * MEMBERS,)),
                pltpu.SemaphoreType.DMA(((BLOCKS - 1) * MEMBERS,)),
                pltpu.SemaphoreType.DMA((MEMBERS,)),
                pltpu.SemaphoreType.DMA((MEMBERS,)),
            ],
            compiler_params=pltpu.CompilerParams(collective_id=0, has_side_effects=True),
        )(*(jnp.transpose(x, (1, 2, 0)) for x in (q_local, k_local, v_local)))
        return jnp.transpose(out_cols, (2, 0, 1))

    return jax.shard_map(
        local_attention, mesh=mesh, in_specs=(seq_spec, seq_spec, seq_spec), out_specs=seq_spec, check_vma=False
    )
```

```python
import functools
import math

import jax
import jax.numpy as jnp
from jax import lax
from jax.experimental import pallas as pl
from jax.experimental.pallas import tpu as pltpu
from jax.sharding import PartitionSpec as P

F32 = jnp.float32
BF16 = jnp.bfloat16
MESH = pl.DeviceIdType.MESH

TILE = 256
MEMBERS = 8
BLOCKS = 4
ROWS = 64
CHUNK = 512
PIECES = CHUNK // ROWS


def flip(value):
    return value + 1 - 2 * lax.rem(value, 2)


class Place:
    def __init__(self, size_x, size_y):
        self.ix, self.iy = lax.axis_index("cx"), lax.axis_index("cy")
        self.size_x, self.size_y = size_x, size_y
        self.chip_x, self.core = self.ix // 2, lax.rem(self.ix, 2)
        self.my_head = self.head_of(self.chip_x, self.iy, self.core)
        self.mirror_x = {"cx": (size_x // 2 - 1 - self.chip_x) * 2 + self.core, "cy": self.iy}
        self.mirror_y = {"cx": self.ix, "cy": size_y - 1 - self.iy}

    def head_of(self, x, y, c):
        px = lax.rem(x + x // (self.size_x // 4), 2)
        py = lax.rem(y + y // (self.size_y // 2), 2)
        return px * 4 + py * 2 + c

    def member(self, r):
        x = flip(self.chip_x) if r // 4 else self.chip_x
        y = flip(self.iy) if (r // 2) % 2 else self.iy
        c = flip(self.core) if r % 2 else self.core
        return {"cx": x * 2 + c, "cy": y}, self.head_of(x, y, c)

    def enter(self, mirrors):
        barrier = pltpu.get_barrier_semaphore()
        partners = [self.member(r)[0] for r in range(1, MEMBERS)]
        partners += [self.mirror_x, self.mirror_y] if mirrors else []
        for who in partners:
            pl.semaphore_signal(barrier, inc=1, device_id=who, device_id_type=MESH)
        pl.semaphore_wait(barrier, len(partners))


def remote(src, dst, sent, here, who):
    return pltpu.make_async_remote_copy(
        src_ref=src, dst_ref=dst, send_sem=sent, recv_sem=here, device_id=who, device_id_type=MESH
    )


def gather_kernel(
    size_x, size_y, q_ref, k_ref, v_ref, q_got, kv_got, kv_sent, kv_here, q_sent, q_here, fwd_sent, fwd_here
):
    place = Place(size_x, size_y)
    head_dim = k_ref.shape[1]
    group = q_ref.shape[0] // k_ref.shape[0]
    place.enter(True)
    member, my_head, mirror_x, mirror_y = place.member, place.my_head, place.mirror_x, place.mirror_y

    def send_kv(k_src, v_src, slot, sent, here, who):
        remote(k_src, slot.at[pl.ds(0, head_dim)], sent, here, who).start()
        remote(v_src, slot.at[pl.ds(head_dim, head_dim)], sent, here, who).start()

    def kv_whole(r):
        slot = kv_got.at[0, r]
        return remote(slot, slot, kv_sent.at[r], kv_here.at[r], member(r)[0])

    def q_copy(r):
        who, head = member(r)
        return remote(q_ref.at[pl.ds(head * group, group)], q_got.at[r], q_sent.at[r], q_here.at[r], who)

    def forward(block, r):
        index = (block - 1) * MEMBERS + r
        if block == 3:
            src, who = (kv_got.at[1, r], mirror_y) if r < 4 else (kv_got.at[2, r], mirror_x)
        else:
            src, who = kv_got.at[0, r], mirror_x if block == 1 else mirror_y
        return remote(src, kv_got.at[block, r], fwd_sent.at[index], fwd_here.at[index], who)

    for r in range(1, MEMBERS):
        who, head = member(r)
        send_kv(k_ref.at[head], v_ref.at[head], kv_got.at[0, r], kv_sent.at[r], kv_here.at[r], who)
    for block, who in ((1, mirror_x), (2, mirror_y)):
        index = (block - 1) * MEMBERS
        send_kv(k_ref.at[my_head], v_ref.at[my_head], kv_got.at[block, 0], fwd_sent.at[index], fwd_here.at[index], who)
    for r in range(1, MEMBERS):
        q_copy(r).start()
    kv_got[0, 0, pl.ds(0, head_dim)] = k_ref[my_head]
    kv_got[0, 0, pl.ds(head_dim, head_dim)] = v_ref[my_head]
    for g in range(group):
        q_got[0, g] = q_ref[my_head * group + g]
    for r in range(1, MEMBERS):
        kv_whole(r).wait_recv()
        forward(1, r).start()
        forward(2, r).start()
    for m in range(4):
        forward(1, m).wait_recv()
        forward(3, m).start()
    for m in range(4, MEMBERS):
        forward(2, m).wait_recv()
        forward(3, m).start()
    for r in range(1, MEMBERS):
        q_copy(r).wait()
        kv_whole(r).wait_send()
    for block in range(1, BLOCKS):
        for r in range(MEMBERS):
            if (block, r // 4) not in ((1, 0), (2, 1)):
                forward(block, r).wait_recv()
            forward(block, r).wait_send()


def return_kernel(size_x, size_y, o_ref, out_ref, out_sent, out_here):
    place = Place(size_x, size_y)
    group = o_ref.shape[1]
    place.enter(False)

    def out_copy(r, head):
        return remote(
            o_ref.at[r], out_ref.at[pl.ds(head * group, group)], out_sent.at[r], out_here.at[r], place.member(r)[0]
        )

    for r in range(1, MEMBERS):
        out_copy(r, place.my_head).start()
    for g in range(group):
        out_ref[place.my_head * group + g] = o_ref[0, g]
    for r in range(1, MEMBERS):
        out_copy(r, place.member(r)[1]).wait_recv()
        out_copy(r, place.my_head).wait_send()


def attend_kernel(
    scale, q_got, kv_got, out_ref, keys, q_limbs, scores, block_max, row_max, row_sum, rescale, acc
):
    group, head_dim, tokens = q_got.shape[1:]
    tiles = group * tokens // TILE
    per_tile = TILE // tokens
    chunks = BLOCKS * MEMBERS * tokens // CHUNK
    steps = MEMBERS * chunks

    def prepare_keys(n, carry):
        columns = kv_got[n // MEMBERS, lax.rem(n, MEMBERS), :head_dim]
        base = pl.multiple_of(n * tokens, tokens)
        keys[pl.ds(base, tokens)] = jnp.transpose(jnp.concatenate([columns, columns], axis=0))
        return carry

    def prepare_queries(r, carry):
        for g in range(group):
            wide = q_got[r, g].astype(F32) * scale
            high = wide.astype(BF16)
            rest = wide - high.astype(F32)
            middle = rest.astype(BF16)
            low = (rest - middle.astype(F32)).astype(BF16)
            cols = pl.ds(g % per_tile * tokens, tokens)
            for n, term in enumerate((high, middle, low)):
                q_limbs[r, g // per_tile, pl.ds(n * head_dim, head_dim), cols] = term
        return carry

    row_max[...] = jnp.full_like(row_max, -jnp.inf)
    row_sum[...] = jnp.zeros_like(row_sum)
    acc[...] = jnp.zeros_like(acc)
    q_limbs[:, :, pl.ds(3 * head_dim, TILE - 3 * head_dim)] = jnp.zeros(
        (MEMBERS, tiles, TILE - 3 * head_dim, TILE), BF16
    )
    lax.fori_loop(0, BLOCKS * MEMBERS, prepare_keys, 0, unroll=8)
    lax.fori_loop(0, MEMBERS, prepare_queries, 0, unroll=2)

    def step_q(i):
        return i // chunks

    def step_c(i):
        return lax.rem(i, chunks)

    def attend(*refs):
        s_acc = (refs[:PIECES], refs[PIECES:2 * PIECES])
        o_acc = refs[2 * PIECES:]

        def push_queries(i):
            for t in range(2):
                pltpu.matmul_push_rhs(q_limbs[step_q(i), t], staging_register=0, mxu_index=t)

        def score_piece(i, k):
            rows = pl.ds(pl.multiple_of(step_c(i) * CHUNK + k * ROWS, ROWS), ROWS)
            doubled = keys[rows]
            lhs = jnp.concatenate([doubled, doubled], axis=1)
            for t in range(2):
                pltpu.matmul_acc_lhs(s_acc[t][k], lhs, load_staged_rhs=0 if k == 0 else None)

        def pop_piece(k, largest):
            result = []
            for t in range(2):
                s = pltpu.matmul_pop(s_acc[t][k])
                scores[t, pl.ds(k * ROWS, ROWS)] = s
                top = jnp.max(s.reshape(ROWS // 8, 8, TILE), axis=0)
                result.append(top if largest is None else jnp.maximum(largest[t], top))
            return result

        def values_lhs(i, part):
            c = step_c(i)
            n = 4 * lax.rem(c, 2) + 2 * part
            return jnp.concatenate([kv_got[c // 2, n + m, pl.ds(head_dim, head_dim)] for m in range(2)], axis=1)

        def weigh(i):
            for t in range(2):
                pltpu.matmul_acc_lhs(o_acc[t], values_lhs(i, 1), load_staged_rhs=0)
            for t in range(2):
                pltpu.matmul_acc_lhs(o_acc[t], values_lhs(i, 0), load_staged_rhs=1)

        def add_weighted(i):
            r = step_q(i)
            for t in range(2):
                acc[r, t] = acc[r, t] * rescale[t][0:1] + pltpu.matmul_pop(o_acc[t])

        def body(i, more_scores=True, more_pops=True):
            before = jnp.maximum(i - 1, 0)
            weigh(before)
            if more_scores:
                push_queries(i + 2)
            r = step_q(i)
            new_max, factor, total = [], [], []
            for t in range(2):
                old = row_max[r, t]
                new = jnp.maximum(old, jnp.max(block_max[t], axis=0, keepdims=True))
                row_max[r, t] = new
                new_max.append(new)
                factor.append(jnp.exp2(old - new))
                total.append(row_sum[r, t] * factor[t])
            largest = None
            probs = [[], []]
            for k in range(PIECES):
                for t in range(2):
                    s = scores[t, pl.ds(k * ROWS, ROWS)].reshape(ROWS // 8, 8, TILE)
                    p = jnp.exp2(s - new_max[t][None])
                    total[t] = total[t] + jnp.sum(p, axis=0)
                    probs[t].append(p.reshape(ROWS, TILE).astype(BF16))
                if more_pops:
                    largest = pop_piece(k, largest)
                if more_scores:
                    score_piece(i + 2, k)
                if k == PIECES // 2 - 1:
                    for t in range(2):
                        pltpu.matmul_push_rhs(jnp.concatenate(probs[t], axis=0), staging_register=1, mxu_index=t)
                    probs = [[], []]
            add_weighted(before)
            for t in range(2):
                pltpu.matmul_push_rhs(jnp.concatenate(probs[t], axis=0), staging_register=0, mxu_index=t)
                row_sum[r, t] = total[t]
                rescale[t] = factor[t]
                if more_pops:
                    block_max[t] = largest[t]

        push_queries(0)
        for k in range(PIECES):
            score_piece(0, k)
        push_queries(1)
        largest = None
        for k in range(PIECES):
            largest = pop_piece(k, largest)
            score_piece(1, k)
        for t in range(2):
            block_max[t] = largest[t]
            rescale[t] = jnp.ones((8, TILE), F32)
            nothing = jnp.zeros((TILE, TILE), BF16)
            pltpu.matmul_push_rhs(nothing, staging_register=1, mxu_index=t)
            pltpu.matmul_push_rhs(nothing, staging_register=0, mxu_index=t)

        def one(i, carry):
            body(i)
            return carry

        lax.fori_loop(0, steps - 2, one, 0)
        body(steps - 2, more_scores=False)
        body(steps - 1, more_scores=False, more_pops=False)
        weigh(steps - 1)
        add_weighted(steps - 1)

    pl.run_scoped(
        attend,
        *([pltpu.ACC(0)((ROWS, TILE), F32)] * PIECES),
        *([pltpu.ACC(1)((ROWS, TILE), F32)] * PIECES),
        pltpu.ACC(0)((head_dim, TILE), F32),
        pltpu.ACC(1)((head_dim, TILE), F32),
    )

    def finish(r, carry):
        for t in range(tiles):
            inverse = 1.0 / jnp.sum(row_sum[r, t], axis=0, keepdims=True)
            result = (acc[r, t] * inverse).astype(BF16)
            for n in range(per_tile):
                out_ref[r, t * per_tile + n] = result[:, n * tokens:(n + 1) * tokens]
        return carry

    lax.fori_loop(0, MEMBERS, finish, 0, unroll=2)


def solution(mesh):
    size_x = mesh.shape["cx"]
    size_y = mesh.shape["cy"]
    seq_spec = P(("batch", "cx", "cy"), None, None)

    def local_attention(q_local, k_local, v_local):
        tokens, num_heads, head_dim = q_local.shape
        num_kv = k_local.shape[1]
        group = num_heads // num_kv
        tiles = group * tokens // TILE
        keys_all = BLOCKS * MEMBERS * tokens
        scale = 1.0 / math.sqrt(head_dim) / math.log(2.0)
        vmem = pl.BlockSpec(memory_space=pltpu.VMEM)
        pieces = jax.ShapeDtypeStruct((MEMBERS, group, head_dim, tokens), BF16)
        dma = pltpu.SemaphoreType.DMA
        q_got, kv_got = pl.pallas_call(
            functools.partial(gather_kernel, size_x, size_y),
            out_shape=[pieces, jax.ShapeDtypeStruct((BLOCKS, MEMBERS, 2 * head_dim, tokens), BF16)],
            in_specs=[vmem] * 3,
            out_specs=[vmem] * 2,
            scratch_shapes=[dma((MEMBERS,))] * 4 + [dma(((BLOCKS - 1) * MEMBERS,))] * 2,
            compiler_params=pltpu.CompilerParams(collective_id=0, has_side_effects=True),
        )(*(jnp.transpose(x, (1, 2, 0)) for x in (q_local, k_local, v_local)))
        owned = pl.pallas_call(
            functools.partial(attend_kernel, scale),
            out_shape=pieces,
            in_specs=[vmem] * 2,
            out_specs=vmem,
            scratch_shapes=[
                pltpu.VMEM((keys_all, 2 * head_dim), BF16),
                pltpu.VMEM((MEMBERS, tiles, TILE, TILE), BF16),
                pltpu.VMEM((tiles, CHUNK, TILE), F32),
                pltpu.VMEM((tiles, 8, TILE), F32),
                pltpu.VMEM((MEMBERS, tiles, 8, TILE), F32),
                pltpu.VMEM((MEMBERS, tiles, 8, TILE), F32),
                pltpu.VMEM((tiles, 8, TILE), F32),
                pltpu.VMEM((MEMBERS, tiles, head_dim, TILE), F32),
            ],
            compiler_params=pltpu.CompilerParams(

            ),
        )(q_got, kv_got)
        out_cols = pl.pallas_call(
            functools.partial(return_kernel, size_x, size_y),
            out_shape=jax.ShapeDtypeStruct((num_heads, head_dim, tokens), BF16),
            in_specs=[vmem],
            out_specs=vmem,
            scratch_shapes=[dma((MEMBERS,))] * 2,
            compiler_params=pltpu.CompilerParams(collective_id=1, has_side_effects=True),
        )(owned)
        return jnp.transpose(out_cols, (2, 0, 1))

    return jax.shard_map(
        local_attention, mesh=mesh, in_specs=(seq_spec, seq_spec, seq_spec), out_specs=seq_spec, check_vma=False
    )
```

```python
import functools
import math

import jax
import jax.numpy as jnp
from jax import lax
from jax.experimental import pallas as pl
from jax.experimental.pallas import tpu as pltpu
from jax.sharding import PartitionSpec as P

F32 = jnp.float32
BF16 = jnp.bfloat16
MESH = pl.DeviceIdType.MESH

TILE = 256
MEMBERS = 8
BLOCKS = 4
ORDER = (
    ((0, 0), (1, 0), (2, 0), (3, 0), (4, 0), (5, 0))
    + ((2, 1), (3, 1), (4, 1), (5, 1), (6, 0), (7, 0))
    + ((7, 1), (7, 2), (7, 3), (6, 1), (6, 2), (6, 3), (5, 2), (5, 3), (3, 2), (3, 3))
    + ((4, 2), (4, 3), (2, 2), (2, 3), (1, 1), (1, 2), (1, 3), (0, 1), (0, 2), (0, 3))
)


def flip(value):
    return value + 1 - 2 * lax.rem(value, 2)


def attend_kernel(
    size_x, size_y, scale,
    q_hbm, k_hbm, v_hbm, out_ref,
    q_ref, k_ref, v_ref, q_got, kv_got, keys, q_limbs, scores, block_max, row_max, row_sum, acc, out_send,
    staged, kv_sent, kv_here, q_sent, q_here, fwd_sent, fwd_here, out_sent, out_here,
):
    head_dim, tokens = k_ref.shape[1:]
    group = q_ref.shape[0] // k_ref.shape[0]
    tiles = group * tokens // TILE
    per_tile = TILE // tokens
    span = MEMBERS * tokens

    local = [pltpu.make_async_copy(*pair, staged.at[n]) for n, pair in
             enumerate(((k_hbm, k_ref), (v_hbm, v_ref), (q_hbm, q_ref)))]
    for copy in local:
        copy.start()

    ix = lax.axis_index("cx")
    iy = lax.axis_index("cy")
    chips_x = size_x // 2
    chip_x, core = ix // 2, lax.rem(ix, 2)
    half_x, half_y = chips_x // 2, size_y // 2

    def head_of(x, y, c):
        px = lax.rem(x + x // half_x, 2)
        py = lax.rem(y + y // half_y, 2)
        return px * 4 + py * 2 + c

    def member(r):
        x = flip(chip_x) if r // 4 else chip_x
        y = flip(iy) if (r // 2) % 2 else iy
        c = flip(core) if r % 2 else core
        return {"cx": x * 2 + c, "cy": y}, head_of(x, y, c)

    my_head = head_of(chip_x, iy, core)
    mirror_x = {"cx": (chips_x - 1 - chip_x) * 2 + core, "cy": iy}
    mirror_y = {"cx": ix, "cy": size_y - 1 - iy}

    barrier = pltpu.get_barrier_semaphore()
    partners = [member(r)[0] for r in range(1, MEMBERS)] + [mirror_x, mirror_y]
    for who in partners:
        pl.semaphore_signal(barrier, inc=1, device_id=who, device_id_type=MESH)
    pl.semaphore_wait(barrier, len(partners))

    def remote(src, dst, sent, here, who):
        return pltpu.make_async_remote_copy(
            src_ref=src, dst_ref=dst, send_sem=sent, recv_sem=here, device_id=who, device_id_type=MESH
        )

    def send_kv(k_src, v_src, slot, sent, here, who):
        remote(k_src, slot.at[pl.ds(0, head_dim)], sent, here, who).start()
        remote(v_src, slot.at[pl.ds(head_dim, head_dim)], sent, here, who).start()

    def kv_whole(r):
        slot = kv_got.at[0, r]
        return remote(slot, slot, kv_sent.at[r], kv_here.at[r], member(r)[0])

    def q_copy(r):
        who, head = member(r)
        return remote(q_ref.at[pl.ds(head * group, group)], q_got.at[r], q_sent.at[r], q_here.at[r], who)

    def forward(block, r):
        index = (block - 1) * MEMBERS + r
        if block == 3:
            src, who = (kv_got.at[1, r], mirror_y) if r < 4 else (kv_got.at[2, r], mirror_x)
        else:
            src, who = kv_got.at[0, r], mirror_x if block == 1 else mirror_y
        return remote(src, kv_got.at[block, r], fwd_sent.at[index], fwd_here.at[index], who)

    def out_copy(r, head):
        return remote(
            out_send.at[r], out_ref.at[pl.ds(head * group, group)], out_sent.at[r], out_here.at[r], member(r)[0]
        )

    local[0].wait()
    local[1].wait()
    for r in range(1, MEMBERS):
        who, head = member(r)
        send_kv(k_ref.at[head], v_ref.at[head], kv_got.at[0, r], kv_sent.at[r], kv_here.at[r], who)
    for block, who in ((1, mirror_x), (2, mirror_y)):
        index = (block - 1) * MEMBERS
        send_kv(k_ref.at[my_head], v_ref.at[my_head], kv_got.at[block, 0], fwd_sent.at[index], fwd_here.at[index], who)
    local[2].wait()
    for r in range(1, MEMBERS):
        q_copy(r).start()

    def prepare_keys(block, r, columns):
        base = block * span + r * tokens
        keys[pl.ds(base, tokens)] = jnp.transpose(jnp.concatenate([columns, columns], axis=0))

    def prepare_queries(r, read):
        for g in range(group):
            wide = read(g).astype(F32) * scale
            high = wide.astype(BF16)
            rest = wide - high.astype(F32)
            middle = rest.astype(BF16)
            low = (rest - middle.astype(F32)).astype(BF16)
            cols = pl.ds(g % per_tile * tokens, tokens)
            for n, term in enumerate((high, middle, low)):
                q_limbs[r, g // per_tile, pl.ds(n * head_dim, head_dim), cols] = term

    def score(r, b):
        doubled = keys[pl.ds(b * span, span)]
        lhs = jnp.concatenate([doubled, doubled], axis=1)
        for t in range(tiles):
            s = jnp.dot(lhs, q_limbs[r, t], preferred_element_type=F32)
            scores[t] = s
            block_max[t] = jnp.max(s.reshape(span // 8, 8, TILE), axis=0)

    def step(r, b, following):
        probs, factors = [], []
        for t in range(tiles):
            old = row_max[r, t]
            new = jnp.maximum(old, jnp.max(block_max[t], axis=0, keepdims=True))
            row_max[r, t] = new
            factors.append(jnp.exp2(old - new))
            p = jnp.exp2(scores[t].reshape(span // 8, 8, TILE) - new[None])
            row_sum[r, t] = row_sum[r, t] * factors[t] + jnp.sum(p, axis=0)
            probs.append(p.reshape(span, TILE).astype(BF16))
        if following:
            score(*following)
        values = jnp.concatenate([kv_got[b, m, pl.ds(head_dim, head_dim)] for m in range(MEMBERS)], axis=1)
        for t in range(tiles):
            weighted = jnp.dot(values, probs[t], preferred_element_type=F32)
            acc[r, t] = acc[r, t] * factors[t][0:1] + weighted

    def finish(r):
        for t in range(tiles):
            inverse = 1.0 / jnp.sum(row_sum[r, t], axis=0, keepdims=True)
            result = (acc[r, t] * inverse).astype(BF16)
            for n in range(per_tile):
                out_send[r, t * per_tile + n] = result[:, n * tokens:(n + 1) * tokens]

    row_max[...] = jnp.full_like(row_max, -jnp.inf)
    row_sum[...] = jnp.zeros_like(row_sum)
    acc[...] = jnp.zeros_like(acc)
    q_limbs[:, :, pl.ds(3 * head_dim, TILE - 3 * head_dim)] = jnp.zeros(
        (MEMBERS, tiles, TILE - 3 * head_dim, TILE), BF16
    )
    prepare_queries(0, lambda g: q_ref[my_head * group + g])
    prepare_keys(0, 0, k_ref[my_head])
    kv_got[0, 0, pl.ds(head_dim, head_dim)] = v_ref[my_head]

    for some in ((1,), (2, 3, 4, 5), (6, 7)):
        for r in some:
            kv_whole(r).wait_recv()
            forward(1, r).start()
            forward(2, r).start()
        for r in some:
            prepare_keys(0, r, kv_got[0, r, :head_dim])

    ready_q, ready_b = {0}, {0}

    def require(n):
        r, b = ORDER[n]
        if r not in ready_q:
            ready_q.add(r)
            q_copy(r).wait_recv()
            prepare_queries(r, lambda g: q_got[r, g])
        if n == 3:
            for m in range(4):
                forward(1, m).wait_recv()
                forward(3, m).start()
        if n == 6:
            for m in range(4, MEMBERS):
                forward(2, m).wait_recv()
                forward(3, m).start()
        if b not in ready_b:
            ready_b.add(b)
            for m in range(MEMBERS):
                if (b, m // 4) not in ((1, 0), (2, 1)):
                    forward(b, m).wait_recv()
            for m in range(MEMBERS):
                prepare_keys(b, m, kv_got[b, m, :head_dim])

    last = {r: n for n, (r, b) in enumerate(ORDER)}
    score(*ORDER[0])
    pending = None
    for n, (r, b) in enumerate(ORDER):
        following = ORDER[n + 1] if n + 1 < len(ORDER) else None
        if following:
            require(n + 1)
        step(r, b, following)
        if pending is not None:
            out_copy(pending, my_head).start()
            pending = None
        if last[r] == n:
            finish(r)
            pending = r if r else None
    mine = pltpu.make_async_copy(out_send.at[0], out_ref.at[pl.ds(my_head * group, group)], out_sent.at[0])
    mine.start()

    for r in range(1, MEMBERS):
        out_copy(r, member(r)[1]).wait_recv()
        out_copy(r, my_head).wait_send()
        kv_whole(r).wait_send()
        q_copy(r).wait_send()
    for block in range(1, BLOCKS):
        for r in range(MEMBERS):
            forward(block, r).wait_send()
    mine.wait()


def solution(mesh):
    size_x = mesh.shape["cx"]
    size_y = mesh.shape["cy"]
    seq_spec = P(("batch", "cx", "cy"), None, None)

    def local_attention(q_local, k_local, v_local):
        tokens, num_heads, head_dim = q_local.shape
        num_kv = k_local.shape[1]
        group = num_heads // num_kv
        tiles = group * tokens // TILE
        span = MEMBERS * tokens
        scale = 1.0 / math.sqrt(head_dim) / math.log(2.0)
        hbm = pl.BlockSpec(memory_space=pl.ANY)
        out_cols = pl.pallas_call(
            functools.partial(attend_kernel, size_x, size_y, scale),
            out_shape=jax.ShapeDtypeStruct((num_heads, head_dim, tokens), BF16),
            in_specs=[hbm] * 3,
            out_specs=hbm,
            scratch_shapes=[
                pltpu.VMEM((num_heads, head_dim, tokens), BF16),
                pltpu.VMEM((num_kv, head_dim, tokens), BF16),
                pltpu.VMEM((num_kv, head_dim, tokens), BF16),
                pltpu.VMEM((MEMBERS, group, head_dim, tokens), BF16),
                pltpu.VMEM((BLOCKS, MEMBERS, 2 * head_dim, tokens), BF16),
                pltpu.VMEM((BLOCKS * span, 2 * head_dim), BF16),
                pltpu.VMEM((MEMBERS, tiles, TILE, TILE), BF16),
                pltpu.VMEM((tiles, span, TILE), F32),
                pltpu.VMEM((tiles, 8, TILE), F32),
                pltpu.VMEM((MEMBERS, tiles, 8, TILE), F32),
                pltpu.VMEM((MEMBERS, tiles, 8, TILE), F32),
                pltpu.VMEM((MEMBERS, tiles, head_dim, TILE), F32),
                pltpu.VMEM((MEMBERS, group, head_dim, tokens), BF16),
                pltpu.SemaphoreType.DMA((3,)),
                pltpu.SemaphoreType.DMA((MEMBERS,)),
                pltpu.SemaphoreType.DMA((MEMBERS,)),
                pltpu.SemaphoreType.DMA((MEMBERS,)),
                pltpu.SemaphoreType.DMA((MEMBERS,)),
                pltpu.SemaphoreType.DMA(((BLOCKS - 1) * MEMBERS,)),
                pltpu.SemaphoreType.DMA(((BLOCKS - 1) * MEMBERS,)),
                pltpu.SemaphoreType.DMA((MEMBERS,)),
                pltpu.SemaphoreType.DMA((MEMBERS,)),
            ],
            compiler_params=pltpu.CompilerParams(
                collective_id=0,
                has_side_effects=True,
            ),
        )(*(jnp.transpose(x, (1, 2, 0)) for x in (q_local, k_local, v_local)))
        return jnp.transpose(out_cols, (2, 0, 1))

    return jax.shard_map(
        local_attention, mesh=mesh, in_specs=(seq_spec, seq_spec, seq_spec), out_specs=seq_spec, check_vma=False
    )
```

```python
import functools
import math

import jax
import jax.numpy as jnp
from jax import lax
from jax.experimental import pallas as pl
from jax.experimental.pallas import tpu as pltpu
from jax.sharding import PartitionSpec as P

F32 = jnp.float32
BF16 = jnp.bfloat16
MESH = pl.DeviceIdType.MESH

TILE = 256
MEMBERS = 8
BLOCKS = 4
ORDER = (
    ((0, 0), (1, 0), (4, 0), (2, 0), (4, 1), (2, 1), (5, 0), (3, 0), (5, 1), (3, 1), (6, 0), (7, 0))
    + ((7, 1), (7, 2), (6, 1), (6, 2), (7, 3), (6, 3), (5, 2), (5, 3), (3, 2), (3, 3), (4, 2), (4, 3), (2, 2), (2, 3))
    + ((1, 1), (1, 2), (1, 3), (0, 1), (0, 2), (0, 3))
)
KEYS, VALUES = 0, 1
RELAYS = {3: (KEYS, 1), 4: (VALUES, 1), 5: (KEYS, 2), 6: (VALUES, 2)}


def flip(value):
    return value + 1 - 2 * lax.rem(value, 2)


def attend_kernel(
    size_x, size_y, scale,
    q_hbm, k_hbm, v_hbm, out_ref,
    q_ref, k_ref, v_ref, q_got, kv_got, keys, q_limbs, scores, block_max, row_max, row_sum, acc, out_send,
    staged, kv_sent, kv_here, q_sent, q_here, fwd_sent, fwd_here, out_sent, out_here,
):
    head_dim, tokens = k_ref.shape[1:]
    group = q_ref.shape[0] // k_ref.shape[0]
    tiles = group * tokens // TILE
    per_tile = TILE // tokens
    span = MEMBERS * tokens

    local = [pltpu.make_async_copy(*pair, staged.at[n]) for n, pair in
             enumerate(((k_hbm, k_ref), (v_hbm, v_ref), (q_hbm, q_ref)))]
    for copy in local:
        copy.start()

    ix = lax.axis_index("cx")
    iy = lax.axis_index("cy")
    chips_x = size_x // 2
    chip_x, core = ix // 2, lax.rem(ix, 2)
    half_x, half_y = chips_x // 2, size_y // 2

    def head_of(x, y, c):
        px = lax.rem(x + x // half_x, 2)
        py = lax.rem(y + y // half_y, 2)
        return px * 4 + py * 2 + c

    def member(r):
        x = flip(chip_x) if r // 4 else chip_x
        y = flip(iy) if (r // 2) % 2 else iy
        c = flip(core) if r % 2 else core
        return {"cx": x * 2 + c, "cy": y}, head_of(x, y, c)

    my_head = head_of(chip_x, iy, core)
    mirror_x = {"cx": (chips_x - 1 - chip_x) * 2 + core, "cy": iy}
    mirror_y = {"cx": ix, "cy": size_y - 1 - iy}

    barrier = pltpu.get_barrier_semaphore()
    partners = [member(r)[0] for r in range(1, MEMBERS)] + [mirror_x, mirror_y]
    for who in partners:
        pl.semaphore_signal(barrier, inc=1, device_id=who, device_id_type=MESH)
    pl.semaphore_wait(barrier, len(partners))

    def remote(src, dst, sent, here, who):
        return pltpu.make_async_remote_copy(
            src_ref=src, dst_ref=dst, send_sem=sent, recv_sem=here, device_id=who, device_id_type=MESH
        )

    def kv_copy(kind, r):
        who, head = member(r)
        src = (k_ref, v_ref)[kind].at[head]
        return remote(src, kv_got.at[kind, 0, r], kv_sent.at[kind, r], kv_here.at[kind, r], who)

    def q_copy(r):
        who, head = member(r)
        return remote(q_ref.at[pl.ds(head * group, group)], q_got.at[r], q_sent.at[r], q_here.at[r], who)

    def forward(kind, block, r):
        index = (block - 1) * MEMBERS + r
        if block == 3:
            src, who = (kv_got.at[kind, 1, r], mirror_y) if r < 4 else (kv_got.at[kind, 2, r], mirror_x)
        else:
            src = kv_got.at[kind, 0, r] if r else (k_ref, v_ref)[kind].at[my_head]
            who = mirror_x if block == 1 else mirror_y
        return remote(src, kv_got.at[kind, block, r], fwd_sent.at[kind, index], fwd_here.at[kind, index], who)

    def out_copy(r, head):
        return remote(
            out_send.at[r], out_ref.at[pl.ds(head * group, group)], out_sent.at[r], out_here.at[r], member(r)[0]
        )

    for kind in (KEYS, VALUES):
        local[kind].wait()
        for r in range(1, MEMBERS):
            kv_copy(kind, r).start()
        forward(kind, 1, 0).start()
        forward(kind, 2, 0).start()
    local[2].wait()
    for r in (1, 4, 2, 5, 3, 6, 7):
        q_copy(r).start()

    def prepare_keys(block, r, columns):
        base = block * span + r * tokens
        keys[pl.ds(base, tokens)] = jnp.transpose(jnp.concatenate([columns, columns], axis=0))

    def prepare_queries(r, read):
        for g in range(group):
            wide = read(g).astype(F32) * scale
            high = wide.astype(BF16)
            rest = wide - high.astype(F32)
            middle = rest.astype(BF16)
            low = (rest - middle.astype(F32)).astype(BF16)
            cols = pl.ds(g % per_tile * tokens, tokens)
            for n, term in enumerate((high, middle, low)):
                q_limbs[r, g // per_tile, pl.ds(n * head_dim, head_dim), cols] = term

    def score(r, b):
        doubled = keys[pl.ds(b * span, span)]
        lhs = jnp.concatenate([doubled, doubled], axis=1)
        for t in range(tiles):
            s = jnp.dot(lhs, q_limbs[r, t], preferred_element_type=F32)
            scores[t] = s
            block_max[t] = jnp.max(s.reshape(span // 8, 8, TILE), axis=0)

    def step(r, b, following):
        probs, factors = [], []
        for t in range(tiles):
            old = row_max[r, t]
            new = jnp.maximum(old, jnp.max(block_max[t], axis=0, keepdims=True))
            row_max[r, t] = new
            factors.append(jnp.exp2(old - new))
            p = jnp.exp2(scores[t].reshape(span // 8, 8, TILE) - new[None])
            row_sum[r, t] = row_sum[r, t] * factors[t] + jnp.sum(p, axis=0)
            probs.append(p.reshape(span, TILE).astype(BF16))
        if following:
            score(*following)
        values = jnp.concatenate([kv_got[VALUES, b, m] for m in range(MEMBERS)], axis=1)
        for t in range(tiles):
            weighted = jnp.dot(values, probs[t], preferred_element_type=F32)
            acc[r, t] = acc[r, t] * factors[t][0:1] + weighted

    def finish(r):
        for t in range(tiles):
            inverse = 1.0 / jnp.sum(row_sum[r, t], axis=0, keepdims=True)
            result = (acc[r, t] * inverse).astype(BF16)
            for n in range(per_tile):
                out_send[r, t * per_tile + n] = result[:, n * tokens:(n + 1) * tokens]

    row_max[...] = jnp.full_like(row_max, -jnp.inf)
    row_sum[...] = jnp.zeros_like(row_sum)
    acc[...] = jnp.zeros_like(acc)
    q_limbs[:, :, pl.ds(3 * head_dim, TILE - 3 * head_dim)] = jnp.zeros(
        (MEMBERS, tiles, TILE - 3 * head_dim, TILE), BF16
    )
    prepare_queries(0, lambda g: q_ref[my_head * group + g])
    prepare_keys(0, 0, k_ref[my_head])
    kv_got[VALUES, 0, 0] = v_ref[my_head]

    for some in ((1,), (2, 3, 4, 5), (6, 7)):
        for r in some:
            kv_copy(KEYS, r).wait_recv()
            forward(KEYS, 1, r).start()
            forward(KEYS, 2, r).start()
        for r in some:
            prepare_keys(0, r, kv_got[KEYS, 0, r])

    ready_q, ready_k, ready_v = {0}, {0}, set()

    def relayed(block, r):
        return (block, r // 4) in ((1, 0), (2, 1))

    def relay(kind, block):
        for m in range(MEMBERS):
            if relayed(block, m):
                forward(kind, block, m).wait_recv()
                forward(kind, 3, m).start()

    def require_scores(n):
        r, b = ORDER[n]
        if r not in ready_q:
            ready_q.add(r)
            q_copy(r).wait_recv()
            prepare_queries(r, lambda g: q_got[r, g])
        if b not in ready_k:
            ready_k.add(b)
            for m in range(MEMBERS):
                if not relayed(b, m):
                    forward(KEYS, b, m).wait_recv()
            for m in range(MEMBERS):
                prepare_keys(b, m, kv_got[KEYS, b, m])

    def require_values(n):
        b = ORDER[n][1]
        if b not in ready_v:
            ready_v.add(b)
            for m in range(MEMBERS):
                if b and not relayed(b, m):
                    forward(VALUES, b, m).wait_recv()
                if not b and m:
                    kv_copy(VALUES, m).wait_recv()
                    forward(VALUES, 1, m).start()
                    forward(VALUES, 2, m).start()

    last = {r: n for n, (r, b) in enumerate(ORDER)}
    score(*ORDER[0])
    pending = None
    for n, (r, b) in enumerate(ORDER):
        following = ORDER[n + 1] if n + 1 < len(ORDER) else None
        if n in RELAYS:
            relay(*RELAYS[n])
        if following:
            require_scores(n + 1)
        require_values(n)
        step(r, b, following)
        if pending is not None:
            out_copy(pending, my_head).start()
            pending = None
        if last[r] == n:
            finish(r)
            pending = r if r else None
    mine = pltpu.make_async_copy(out_send.at[0], out_ref.at[pl.ds(my_head * group, group)], out_sent.at[0])
    mine.start()

    for r in range(1, MEMBERS):
        out_copy(r, member(r)[1]).wait_recv()
        out_copy(r, my_head).wait_send()
        q_copy(r).wait_send()
    for kind in (KEYS, VALUES):
        for r in range(1, MEMBERS):
            kv_copy(kind, r).wait_send()
        for block in range(1, BLOCKS):
            for r in range(MEMBERS):
                forward(kind, block, r).wait_send()
    mine.wait()


def solution(mesh):
    size_x = mesh.shape["cx"]
    size_y = mesh.shape["cy"]
    seq_spec = P(("batch", "cx", "cy"), None, None)

    def local_attention(q_local, k_local, v_local):
        tokens, num_heads, head_dim = q_local.shape
        num_kv = k_local.shape[1]
        group = num_heads // num_kv
        tiles = group * tokens // TILE
        span = MEMBERS * tokens
        scale = 1.0 / math.sqrt(head_dim) / math.log(2.0)
        hbm = pl.BlockSpec(memory_space=pl.ANY)
        out_cols = pl.pallas_call(
            functools.partial(attend_kernel, size_x, size_y, scale),
            out_shape=jax.ShapeDtypeStruct((num_heads, head_dim, tokens), BF16),
            in_specs=[hbm] * 3,
            out_specs=hbm,
            scratch_shapes=[
                pltpu.VMEM((num_heads, head_dim, tokens), BF16),
                pltpu.VMEM((num_kv, head_dim, tokens), BF16),
                pltpu.VMEM((num_kv, head_dim, tokens), BF16),
                pltpu.VMEM((MEMBERS, group, head_dim, tokens), BF16),
                pltpu.VMEM((2, BLOCKS, MEMBERS, head_dim, tokens), BF16),
                pltpu.VMEM((BLOCKS * span, 2 * head_dim), BF16),
                pltpu.VMEM((MEMBERS, tiles, TILE, TILE), BF16),
                pltpu.VMEM((tiles, span, TILE), F32),
                pltpu.VMEM((tiles, 8, TILE), F32),
                pltpu.VMEM((MEMBERS, tiles, 8, TILE), F32),
                pltpu.VMEM((MEMBERS, tiles, 8, TILE), F32),
                pltpu.VMEM((MEMBERS, tiles, head_dim, TILE), F32),
                pltpu.VMEM((MEMBERS, group, head_dim, tokens), BF16),
                pltpu.SemaphoreType.DMA((3,)),
                pltpu.SemaphoreType.DMA((2, MEMBERS)),
                pltpu.SemaphoreType.DMA((2, MEMBERS)),
                pltpu.SemaphoreType.DMA((MEMBERS,)),
                pltpu.SemaphoreType.DMA((MEMBERS,)),
                pltpu.SemaphoreType.DMA((2, (BLOCKS - 1) * MEMBERS)),
                pltpu.SemaphoreType.DMA((2, (BLOCKS - 1) * MEMBERS)),
                pltpu.SemaphoreType.DMA((MEMBERS,)),
                pltpu.SemaphoreType.DMA((MEMBERS,)),
            ],
            compiler_params=pltpu.CompilerParams(
                collective_id=0,
                has_side_effects=True,
            ),
        )(*(jnp.transpose(x, (1, 2, 0)) for x in (q_local, k_local, v_local)))
        return jnp.transpose(out_cols, (2, 0, 1))

    return jax.shard_map(
        local_attention, mesh=mesh, in_specs=(seq_spec, seq_spec, seq_spec), out_specs=seq_spec, check_vma=False
    )
```

```python
import functools
import math

import jax
import jax.numpy as jnp
from jax import lax
from jax.experimental import pallas as pl
from jax.experimental.pallas import tpu as pltpu
from jax.sharding import PartitionSpec as P

F32 = jnp.float32
BF16 = jnp.bfloat16
MESH = pl.DeviceIdType.MESH

TILE = 256
MEMBERS = 8
BLOCKS = 4
ORDER = (
    ((0, 0), (1, 0), (4, 0), (2, 0), (5, 0), (3, 0), (4, 1), (2, 1), (5, 1), (3, 1), (6, 0), (7, 0))
    + ((7, 1), (6, 1), (7, 2), (6, 2), (7, 3), (6, 3), (5, 2), (5, 3), (3, 2), (3, 3), (4, 2), (4, 3), (2, 2), (2, 3))
    + ((1, 1), (1, 2), (1, 3), (0, 1), (0, 2), (0, 3))
)
KEYS, VALUES = 0, 1
RELAYS = {3: (KEYS, 1), 5: (KEYS, 2), 6: (VALUES, 1), 8: (VALUES, 2)}


def attend_kernel(
    size_x, size_y, scale,
    q_hbm, k_hbm, v_hbm, out_ref,
    q_ref, k_ref, v_ref, q_got, kv_got, keys, q_limbs, scores, block_max, row_max, row_sum, acc, out_send,
    staged, kv_sent, kv_here, q_sent, q_here, fwd_sent, fwd_here, out_sent, out_here,
):
    head_dim, tokens = k_ref.shape[1:]
    group = q_ref.shape[0] // k_ref.shape[0]
    tiles = group * tokens // TILE
    per_tile = TILE // tokens
    span = MEMBERS * tokens

    local = [pltpu.make_async_copy(*pair, staged.at[n]) for n, pair in
             enumerate(((k_hbm, k_ref), (v_hbm, v_ref), (q_hbm, q_ref)))]
    for copy in local:
        copy.start()

    ix = lax.axis_index("cx")
    iy = lax.axis_index("cy")
    chips_x = size_x // 2
    chip_x, core = ix // 2, lax.rem(ix, 2)
    half_x, half_y = chips_x // 2, size_y // 2

    def head_of(x, y, c):
        px = lax.rem(x + x // half_x, 2)
        py = lax.rem(y + y // half_y, 2)
        return px * 4 + py * 2 + c

    def member(r):
        x = chip_x + r // 4 * (1 - 2 * lax.rem(chip_x, 2))
        y = iy + r // 2 % 2 * (1 - 2 * lax.rem(iy, 2))
        c = core + r % 2 * (1 - 2 * core)
        return {"cx": x * 2 + c, "cy": y}, head_of(x, y, c)

    my_head = head_of(chip_x, iy, core)
    mirror_x = {"cx": (chips_x - 1 - chip_x) * 2 + core, "cy": iy}
    mirror_y = {"cx": ix, "cy": size_y - 1 - iy}

    barrier = pltpu.get_barrier_semaphore()
    partners = [member(r)[0] for r in range(1, MEMBERS)] + [mirror_x, mirror_y]
    for who in partners:
        pl.semaphore_signal(barrier, inc=1, device_id=who, device_id_type=MESH)
    pl.semaphore_wait(barrier, len(partners))

    def remote(src, dst, sent, here, who):
        return pltpu.make_async_remote_copy(
            src_ref=src, dst_ref=dst, send_sem=sent, recv_sem=here, device_id=who, device_id_type=MESH
        )

    def kv_copy(kind, r):
        who, head = member(r)
        src = (k_ref, v_ref)[kind].at[head]
        return remote(src, kv_got.at[kind, 0, r], kv_sent.at[kind, r], kv_here.at[kind, r], who)

    def q_copy(r):
        who, head = member(r)
        return remote(q_ref.at[pl.ds(head * group, group)], q_got.at[r], q_sent.at[r], q_here.at[r], who)

    def forward(kind, block, r):
        index = (block - 1) * MEMBERS + r
        if block == 3:
            src, who = (kv_got.at[kind, 1, r], mirror_y) if r < 4 else (kv_got.at[kind, 2, r], mirror_x)
        else:
            src = kv_got.at[kind, 0, r] if r else (k_ref, v_ref)[kind].at[my_head]
            who = mirror_x if block == 1 else mirror_y
        return remote(src, kv_got.at[kind, block, r], fwd_sent.at[kind, index], fwd_here.at[kind, index], who)

    def out_copy(r, head):
        return remote(
            out_send.at[r], out_ref.at[pl.ds(head * group, group)], out_sent.at[r], out_here.at[r], member(r)[0]
        )

    for kind in (KEYS, VALUES):
        local[kind].wait()
        for r in range(1, MEMBERS):
            kv_copy(kind, r).start()
        forward(kind, 1, 0).start()
        forward(kind, 2, 0).start()
    local[2].wait()
    for r in (1, 4, 2, 5, 3, 6, 7):
        q_copy(r).start()

    def prepare_keys(block, r, columns):
        base = block * span + r * tokens
        keys[pl.ds(base, tokens)] = jnp.transpose(jnp.concatenate([columns, columns], axis=0))

    def prepare_queries(r, read):
        for g in range(group):
            wide = read(g).astype(F32) * scale
            high = wide.astype(BF16)
            rest = wide - high.astype(F32)
            middle = rest.astype(BF16)
            low = (rest - middle.astype(F32)).astype(BF16)
            cols = pl.ds(g % per_tile * tokens, tokens)
            for n, term in enumerate((high, middle, low)):
                q_limbs[r, g // per_tile, pl.ds(n * head_dim, head_dim), cols] = term

    def score(r, b):
        doubled = keys[pl.ds(pl.multiple_of(b * span, span), span)]
        lhs = jnp.concatenate([doubled, doubled], axis=1)
        for t in range(tiles):
            s = jnp.dot(lhs, q_limbs[r, t], preferred_element_type=F32)
            scores[t] = s
            block_max[t] = jnp.max(s.reshape(span // 8, 8, TILE), axis=0)

    def step(r, b, following):
        probs, factors = [], []
        for t in range(tiles):
            old = row_max[r, t]
            new = jnp.maximum(old, jnp.max(block_max[t], axis=0, keepdims=True))
            row_max[r, t] = new
            factors.append(jnp.exp2(old - new))
            p = jnp.exp2(scores[t].reshape(span // 8, 8, TILE) - new[None])
            row_sum[r, t] = row_sum[r, t] * factors[t] + jnp.sum(p, axis=0)
            probs.append(p.reshape(span, TILE).astype(BF16))
        if following is not None:
            score(*following)
        values = jnp.concatenate([kv_got[VALUES, b, m] for m in range(MEMBERS)], axis=1)
        for t in range(tiles):
            weighted = jnp.dot(values, probs[t], preferred_element_type=F32)
            acc[r, t] = acc[r, t] * factors[t][0:1] + weighted

    def finish(r):
        for t in range(tiles):
            inverse = 1.0 / jnp.sum(row_sum[r, t], axis=0, keepdims=True)
            result = (acc[r, t] * inverse).astype(BF16)
            for n in range(per_tile):
                out_send[r, t * per_tile + n] = result[:, n * tokens:(n + 1) * tokens]

    row_max[...] = jnp.full_like(row_max, -jnp.inf)
    row_sum[...] = jnp.zeros_like(row_sum)
    acc[...] = jnp.zeros_like(acc)
    q_limbs[:, :, pl.ds(3 * head_dim, TILE - 3 * head_dim)] = jnp.zeros(
        (MEMBERS, tiles, TILE - 3 * head_dim, TILE), BF16
    )
    prepare_queries(0, lambda g: q_ref[my_head * group + g])
    prepare_keys(0, 0, k_ref[my_head])
    kv_got[VALUES, 0, 0] = v_ref[my_head]

    def values_here(m):
        kv_copy(VALUES, m).wait_recv()
        forward(VALUES, 1, m).start()
        forward(VALUES, 2, m).start()

    for some in ((1,), (2, 3, 4, 5), (6, 7)):
        for r in some:
            kv_copy(KEYS, r).wait_recv()
            forward(KEYS, 1, r).start()
            forward(KEYS, 2, r).start()
            if r == 1:
                values_here(r)
        for r in some:
            prepare_keys(0, r, kv_got[KEYS, 0, r])

    ready_q, ready_k, ready_v = {0}, {0}, set()

    def relayed(block, r):
        return (block, r // 4) in ((1, 0), (2, 1))

    def relay(kind, block):
        for m in range(MEMBERS):
            if relayed(block, m):
                forward(kind, block, m).wait_recv()
                forward(kind, 3, m).start()

    def require_scores(n):
        r, b = ORDER[n]
        if r not in ready_q:
            ready_q.add(r)
            q_copy(r).wait_recv()
            prepare_queries(r, lambda g: q_got[r, g])
        if b not in ready_k:
            ready_k.add(b)
            for m in range(MEMBERS):
                if not relayed(b, m):
                    forward(KEYS, b, m).wait_recv()
            for m in range(MEMBERS):
                prepare_keys(b, m, kv_got[KEYS, b, m])

    def require_values(n):
        b = ORDER[n][1]
        if b not in ready_v:
            ready_v.add(b)
            for m in range(MEMBERS):
                if b and not relayed(b, m):
                    forward(VALUES, b, m).wait_recv()
                if not b and m > 1:
                    values_here(m)

    def coded(n):
        code = 0
        for k, (r, b) in enumerate(ORDER):
            code = jnp.where(n == k, r * BLOCKS + b, code)
        return code // BLOCKS, lax.rem(code, BLOCKS)

    def hooks(n):
        if n in RELAYS:
            relay(*RELAYS[n])
        require_scores(n + 1)
        require_values(n)

    def one(n, carry):
        done_r, done_b, r, b = carry

        @pl.when(done_b == BLOCKS - 1)
        def _():
            out_copy(done_r, my_head).start()

        @pl.when(n < waits)
        def _():
            for k in range(waits):

                @pl.when(n == k)
                def _(k=k):
                    hooks(k)

        following = coded(n + 1)
        step(r, b, following)

        @pl.when(b == BLOCKS - 1)
        def _():
            finish(r)

        return r, b, *following

    waits = 1 + max(
        max(n for n, (r, b) in enumerate(ORDER) if (r, b) == min(p for p in ORDER if p[0] == r)) for r in range(MEMBERS)
    )
    waits = max(waits, 1 + min(n for n, (r, b) in enumerate(ORDER) if b == BLOCKS - 1))
    score(*ORDER[0])
    zero = jnp.int32(0)
    lax.fori_loop(0, len(ORDER) - 1, one, (zero, zero, zero + ORDER[0][0], zero + ORDER[0][1]))
    step(*ORDER[-1], None)
    finish(ORDER[-1][0])
    mine = pltpu.make_async_copy(out_send.at[0], out_ref.at[pl.ds(my_head * group, group)], out_sent.at[0])
    mine.start()

    for r in range(1, MEMBERS):
        out_copy(r, member(r)[1]).wait_recv()
        out_copy(r, my_head).wait_send()
        q_copy(r).wait_send()
    for kind in (KEYS, VALUES):
        for r in range(1, MEMBERS):
            kv_copy(kind, r).wait_send()
        for block in range(1, BLOCKS):
            for r in range(MEMBERS):
                forward(kind, block, r).wait_send()
    mine.wait()


def solution(mesh):
    size_x = mesh.shape["cx"]
    size_y = mesh.shape["cy"]
    seq_spec = P(("batch", "cx", "cy"), None, None)

    def local_attention(q_local, k_local, v_local):
        tokens, num_heads, head_dim = q_local.shape
        num_kv = k_local.shape[1]
        group = num_heads // num_kv
        tiles = group * tokens // TILE
        span = MEMBERS * tokens
        scale = 1.0 / math.sqrt(head_dim) / math.log(2.0)
        hbm = pl.BlockSpec(memory_space=pl.ANY)
        out_cols = pl.pallas_call(
            functools.partial(attend_kernel, size_x, size_y, scale),
            out_shape=jax.ShapeDtypeStruct((num_heads, head_dim, tokens), BF16),
            in_specs=[hbm] * 3,
            out_specs=hbm,
            scratch_shapes=[
                pltpu.VMEM((num_heads, head_dim, tokens), BF16),
                pltpu.VMEM((num_kv, head_dim, tokens), BF16),
                pltpu.VMEM((num_kv, head_dim, tokens), BF16),
                pltpu.VMEM((MEMBERS, group, head_dim, tokens), BF16),
                pltpu.VMEM((2, BLOCKS, MEMBERS, head_dim, tokens), BF16),
                pltpu.VMEM((BLOCKS * span, 2 * head_dim), BF16),
                pltpu.VMEM((MEMBERS, tiles, TILE, TILE), BF16),
                pltpu.VMEM((tiles, span, TILE), F32),
                pltpu.VMEM((tiles, 8, TILE), F32),
                pltpu.VMEM((MEMBERS, tiles, 8, TILE), F32),
                pltpu.VMEM((MEMBERS, tiles, 8, TILE), F32),
                pltpu.VMEM((MEMBERS, tiles, head_dim, TILE), F32),
                pltpu.VMEM((MEMBERS, group, head_dim, tokens), BF16),
                pltpu.SemaphoreType.DMA((3,)),
                pltpu.SemaphoreType.DMA((2, MEMBERS)),
                pltpu.SemaphoreType.DMA((2, MEMBERS)),
                pltpu.SemaphoreType.DMA((MEMBERS,)),
                pltpu.SemaphoreType.DMA((MEMBERS,)),
                pltpu.SemaphoreType.DMA((2, (BLOCKS - 1) * MEMBERS)),
                pltpu.SemaphoreType.DMA((2, (BLOCKS - 1) * MEMBERS)),
                pltpu.SemaphoreType.DMA((MEMBERS,)),
                pltpu.SemaphoreType.DMA((MEMBERS,)),
            ],
            compiler_params=pltpu.CompilerParams(
                collective_id=0,
                has_side_effects=True,
            ),
        )(*(jnp.transpose(x, (1, 2, 0)) for x in (q_local, k_local, v_local)))
        return jnp.transpose(out_cols, (2, 0, 1))

    return jax.shard_map(
        local_attention, mesh=mesh, in_specs=(seq_spec, seq_spec, seq_spec), out_specs=seq_spec, check_vma=False
    )
```

```python
import functools
import math

import jax
import jax.numpy as jnp
from jax import lax
from jax.experimental import pallas as pl
from jax.experimental.pallas import tpu as pltpu
from jax.sharding import PartitionSpec as P

F32 = jnp.float32
BF16 = jnp.bfloat16
MESH = pl.DeviceIdType.MESH

TILE = 256
MEMBERS = 8
BLOCKS = 4
GROUPS = (
    ((0, 0),),
    ((1, 0),),
    ((4, 0),),
    ((2, 0),),
    ((5, 0), (3, 0)),
    ((4, 1), (2, 1), (5, 1)),
    ((3, 1), (6, 0), (7, 0), (7, 1), (6, 1)),
    ((7, 2), (6, 2), (7, 3), (6, 3)),
    ((5, 2), (5, 3), (3, 2), (3, 3)),
    ((4, 2), (4, 3), (2, 2), (2, 3)),
    ((1, 1), (1, 2), (1, 3)),
    ((0, 1), (0, 2), (0, 3)),
)
KEYS, VALUES = 0, 1
RELAYS = {3: ((KEYS, 1),), 4: ((KEYS, 2),), 5: ((VALUES, 1), (VALUES, 2))}


def flip(value):
    return value + 1 - 2 * lax.rem(value, 2)


def attend_kernel(
    size_x, size_y, scale,
    q_hbm, k_hbm, v_hbm, out_ref,
    q_ref, k_ref, v_ref, q_got, kv_got, keys, q_limbs, scores, block_max, row_max, row_sum, acc, out_send,
    staged, kv_sent, kv_here, q_sent, q_here, fwd_sent, fwd_here, out_sent, out_here,
):
    head_dim, tokens = k_ref.shape[1:]
    group = q_ref.shape[0] // k_ref.shape[0]
    tiles = group * tokens // TILE
    per_tile = TILE // tokens
    span = MEMBERS * tokens

    local = [pltpu.make_async_copy(*pair, staged.at[n]) for n, pair in
             enumerate(((k_hbm, k_ref), (v_hbm, v_ref), (q_hbm, q_ref)))]
    for copy in local:
        copy.start()

    ix = lax.axis_index("cx")
    iy = lax.axis_index("cy")
    chips_x = size_x // 2
    chip_x, core = ix // 2, lax.rem(ix, 2)
    half_x, half_y = chips_x // 2, size_y // 2

    def head_of(x, y, c):
        px = lax.rem(x + x // half_x, 2)
        py = lax.rem(y + y // half_y, 2)
        return px * 4 + py * 2 + c

    def member(r):
        x = flip(chip_x) if r // 4 else chip_x
        y = flip(iy) if (r // 2) % 2 else iy
        c = flip(core) if r % 2 else core
        return {"cx": x * 2 + c, "cy": y}, head_of(x, y, c)

    my_head = head_of(chip_x, iy, core)
    mirror_x = {"cx": (chips_x - 1 - chip_x) * 2 + core, "cy": iy}
    mirror_y = {"cx": ix, "cy": size_y - 1 - iy}

    barrier = pltpu.get_barrier_semaphore()
    partners = [member(r)[0] for r in range(1, MEMBERS)] + [mirror_x, mirror_y]
    for who in partners:
        pl.semaphore_signal(barrier, inc=1, device_id=who, device_id_type=MESH)
    pl.semaphore_wait(barrier, len(partners))

    def remote(src, dst, sent, here, who):
        return pltpu.make_async_remote_copy(
            src_ref=src, dst_ref=dst, send_sem=sent, recv_sem=here, device_id=who, device_id_type=MESH
        )

    def kv_copy(kind, r):
        who, head = member(r)
        src = (k_ref, v_ref)[kind].at[head]
        return remote(src, kv_got.at[kind, 0, r], kv_sent.at[kind, r], kv_here.at[kind, r], who)

    def q_copy(r):
        who, head = member(r)
        return remote(q_ref.at[pl.ds(head * group, group)], q_got.at[r], q_sent.at[r], q_here.at[r], who)

    def forward(kind, block, r):
        index = (block - 1) * MEMBERS + r
        if block == 3:
            src, who = (kv_got.at[kind, 1, r], mirror_y) if r < 4 else (kv_got.at[kind, 2, r], mirror_x)
        else:
            src = kv_got.at[kind, 0, r] if r else (k_ref, v_ref)[kind].at[my_head]
            who = mirror_x if block == 1 else mirror_y
        return remote(src, kv_got.at[kind, block, r], fwd_sent.at[kind, index], fwd_here.at[kind, index], who)

    def out_copy(r, head):
        return remote(
            out_send.at[r], out_ref.at[pl.ds(head * group, group)], out_sent.at[r], out_here.at[r], member(r)[0]
        )

    for kind in (KEYS, VALUES):
        local[kind].wait()
        for r in range(1, MEMBERS):
            kv_copy(kind, r).start()
        forward(kind, 1, 0).start()
        forward(kind, 2, 0).start()
    local[2].wait()
    for r in (1, 4, 2, 5, 3, 6, 7):
        q_copy(r).start()

    def prepare_keys(block, r, columns):
        base = block * span + r * tokens
        keys[pl.ds(base, tokens)] = jnp.transpose(jnp.concatenate([columns, columns], axis=0))

    def prepare_queries(r, read):
        for g in range(group):
            wide = read(g).astype(F32) * scale
            high = wide.astype(BF16)
            rest = wide - high.astype(F32)
            middle = rest.astype(BF16)
            low = (rest - middle.astype(F32)).astype(BF16)
            cols = pl.ds(g % per_tile * tokens, tokens)
            for n, term in enumerate((high, middle, low)):
                q_limbs[r, g // per_tile, pl.ds(n * head_dim, head_dim), cols] = term

    def score(r, b):
        doubled = keys[pl.ds(b * span, span)]
        lhs = jnp.concatenate([doubled, doubled], axis=1)
        for t in range(tiles):
            s = jnp.dot(lhs, q_limbs[r, t], preferred_element_type=F32)
            scores[t] = s
            block_max[t] = jnp.max(s.reshape(span // 8, 8, TILE), axis=0)

    def step(r, b, following):
        probs, factors = [], []
        for t in range(tiles):
            old = row_max[r, t]
            new = jnp.maximum(old, jnp.max(block_max[t], axis=0, keepdims=True))
            row_max[r, t] = new
            factors.append(jnp.exp2(old - new))
            p = jnp.exp2(scores[t].reshape(span // 8, 8, TILE) - new[None])
            row_sum[r, t] = row_sum[r, t] * factors[t] + jnp.sum(p, axis=0)
            probs.append(p.reshape(span, TILE).astype(BF16))
        if following:
            score(*following)
        values = jnp.concatenate([kv_got[VALUES, b, m] for m in range(MEMBERS)], axis=1)
        for t in range(tiles):
            weighted = jnp.dot(values, probs[t], preferred_element_type=F32)
            acc[r, t] = acc[r, t] * factors[t][0:1] + weighted

    def finish(r):
        for t in range(tiles):
            inverse = 1.0 / jnp.sum(row_sum[r, t], axis=0, keepdims=True)
            result = (acc[r, t] * inverse).astype(BF16)
            for n in range(per_tile):
                out_send[r, t * per_tile + n] = result[:, n * tokens:(n + 1) * tokens]

    row_max[...] = jnp.full_like(row_max, -jnp.inf)
    row_sum[...] = jnp.zeros_like(row_sum)
    acc[...] = jnp.zeros_like(acc)
    q_limbs[:, :, pl.ds(3 * head_dim, TILE - 3 * head_dim)] = jnp.zeros(
        (MEMBERS, tiles, TILE - 3 * head_dim, TILE), BF16
    )
    prepare_queries(0, lambda g: q_ref[my_head * group + g])
    prepare_keys(0, 0, k_ref[my_head])
    kv_got[VALUES, 0, 0] = v_ref[my_head]

    def values_here(m):
        kv_copy(VALUES, m).wait_recv()
        forward(VALUES, 1, m).start()
        forward(VALUES, 2, m).start()

    for some in ((1,), (2, 3, 4, 5), (6, 7)):
        for r in some:
            kv_copy(KEYS, r).wait_recv()
            forward(KEYS, 1, r).start()
            forward(KEYS, 2, r).start()
            if r == 1:
                values_here(r)
        for r in some:
            prepare_keys(0, r, kv_got[KEYS, 0, r])

    ready_q, ready_k, ready_v = {0}, {0}, set()

    def relayed(block, r):
        return (block, r // 4) in ((1, 0), (2, 1))

    def relay(kind, block):
        for m in range(MEMBERS):
            if relayed(block, m):
                forward(kind, block, m).wait_recv()
                forward(kind, 3, m).start()

    def require_scores(r, b):
        if r not in ready_q:
            ready_q.add(r)
            q_copy(r).wait_recv()
            prepare_queries(r, lambda g: q_got[r, g])
        if b not in ready_k:
            ready_k.add(b)
            for m in range(MEMBERS):
                if not relayed(b, m):
                    forward(KEYS, b, m).wait_recv()
            for m in range(MEMBERS):
                prepare_keys(b, m, kv_got[KEYS, b, m])

    def require_values(b):
        if b not in ready_v:
            ready_v.add(b)
            for m in range(MEMBERS):
                if b and not relayed(b, m):
                    forward(VALUES, b, m).wait_recv()
                if not b and m > 1:
                    values_here(m)

    order = [step for group in GROUPS for step in group]
    last = {r: n for n, (r, b) in enumerate(order)}
    score(*order[0])
    n = 0
    ended = []
    for number, members in enumerate(GROUPS):
        for kind, block in RELAYS.get(number, ()):
            relay(kind, block)
        for following in order[n + 1:n + len(members) + 1]:
            require_scores(*following)
        for r, b in members:
            require_values(b)
        for r in ended:
            out_copy(r, my_head).start()
        ended = []
        for r, b in members:
            step(r, b, order[n + 1] if n + 1 < len(order) else None)
            if last[r] == n:
                finish(r)
                ended += [r] if r else []
            n += 1
    mine = pltpu.make_async_copy(out_send.at[0], out_ref.at[pl.ds(my_head * group, group)], out_sent.at[0])
    mine.start()

    for r in range(1, MEMBERS):
        out_copy(r, member(r)[1]).wait_recv()
        out_copy(r, my_head).wait_send()
        q_copy(r).wait_send()
    for kind in (KEYS, VALUES):
        for r in range(1, MEMBERS):
            kv_copy(kind, r).wait_send()
        for block in range(1, BLOCKS):
            for r in range(MEMBERS):
                forward(kind, block, r).wait_send()
    mine.wait()


def solution(mesh):
    size_x = mesh.shape["cx"]
    size_y = mesh.shape["cy"]
    seq_spec = P(("batch", "cx", "cy"), None, None)

    def local_attention(q_local, k_local, v_local):
        tokens, num_heads, head_dim = q_local.shape
        num_kv = k_local.shape[1]
        group = num_heads // num_kv
        tiles = group * tokens // TILE
        span = MEMBERS * tokens
        scale = 1.0 / math.sqrt(head_dim) / math.log(2.0)
        hbm = pl.BlockSpec(memory_space=pl.ANY)
        out_cols = pl.pallas_call(
            functools.partial(attend_kernel, size_x, size_y, scale),
            out_shape=jax.ShapeDtypeStruct((num_heads, head_dim, tokens), BF16),
            in_specs=[hbm] * 3,
            out_specs=hbm,
            scratch_shapes=[
                pltpu.VMEM((num_heads, head_dim, tokens), BF16),
                pltpu.VMEM((num_kv, head_dim, tokens), BF16),
                pltpu.VMEM((num_kv, head_dim, tokens), BF16),
                pltpu.VMEM((MEMBERS, group, head_dim, tokens), BF16),
                pltpu.VMEM((2, BLOCKS, MEMBERS, head_dim, tokens), BF16),
                pltpu.VMEM((BLOCKS * span, 2 * head_dim), BF16),
                pltpu.VMEM((MEMBERS, tiles, TILE, TILE), BF16),
                pltpu.VMEM((tiles, span, TILE), F32),
                pltpu.VMEM((tiles, 8, TILE), F32),
                pltpu.VMEM((MEMBERS, tiles, 8, TILE), F32),
                pltpu.VMEM((MEMBERS, tiles, 8, TILE), F32),
                pltpu.VMEM((MEMBERS, tiles, head_dim, TILE), F32),
                pltpu.VMEM((MEMBERS, group, head_dim, tokens), BF16),
                pltpu.SemaphoreType.DMA((3,)),
                pltpu.SemaphoreType.DMA((2, MEMBERS)),
                pltpu.SemaphoreType.DMA((2, MEMBERS)),
                pltpu.SemaphoreType.DMA((MEMBERS,)),
                pltpu.SemaphoreType.DMA((MEMBERS,)),
                pltpu.SemaphoreType.DMA((2, (BLOCKS - 1) * MEMBERS)),
                pltpu.SemaphoreType.DMA((2, (BLOCKS - 1) * MEMBERS)),
                pltpu.SemaphoreType.DMA((MEMBERS,)),
                pltpu.SemaphoreType.DMA((MEMBERS,)),
            ],
            compiler_params=pltpu.CompilerParams(
                collective_id=0,
                has_side_effects=True,
            ),
        )(*(jnp.transpose(x, (1, 2, 0)) for x in (q_local, k_local, v_local)))
        return jnp.transpose(out_cols, (2, 0, 1))

    return jax.shard_map(
        local_attention, mesh=mesh, in_specs=(seq_spec, seq_spec, seq_spec), out_specs=seq_spec, check_vma=False
    )
```

```python
import functools
import math

import jax
import jax.numpy as jnp
from jax import lax
from jax.experimental import pallas as pl
from jax.experimental.pallas import tpu as pltpu
from jax.sharding import PartitionSpec as P

F32 = jnp.float32
BF16 = jnp.bfloat16
MESH = pl.DeviceIdType.MESH

TILE = 256
MEMBERS = 8
BLOCKS = 4
SETS = (
    ((0, 0), (0, 1), (0, 2), (0, 3), (0, 4), (0, 5), (1, 0), (2, 0)),
    ((1, 1), (2, 1), (1, 2), (1, 3), (2, 4), (2, 5), (0, 6), (0, 7)),
    ((1, 4), (1, 5), (2, 2), (2, 3), (1, 6), (1, 7), (2, 6), (2, 7)),
    tuple((3, r) for r in range(MEMBERS)),
)
GROUPS = (
    ((0, 0),),
    ((1, 0),),
    ((4, 0),),
    ((2, 0),),
    ((4, 1), (2, 1)),
    ((5, 0), (3, 0), (5, 1)),
    ((3, 1),),
    ((6, 0), (6, 1)),
    ((6, 2), (7, 0), (7, 1), (7, 2)),
    ((7, 3), (6, 3)),
    ((5, 2), (5, 3), (3, 2), (3, 3)),
    ((4, 2), (4, 3), (2, 2), (2, 3)),
    ((1, 1), (1, 2), (1, 3)),
    ((0, 1), (0, 2), (0, 3)),
)
KEYS, VALUES = 0, 1
RELAYS = {1: ((1, 0), (1, 1)), 4: ((1, 2), (1, 3), (2, 4), (2, 5)), 6: ((2, 6), (2, 7))}


def flip(value):
    return value + 1 - 2 * lax.rem(value, 2)


def attend_kernel(
    size_x, size_y, scale,
    q_hbm, k_hbm, v_hbm, out_ref,
    q_ref, k_ref, v_ref, q_got, kv_got, keys, q_limbs, scores, block_max, row_max, row_sum, acc, out_send,
    staged, kv_sent, kv_here, q_sent, q_here, fwd_sent, fwd_here, out_sent, out_here,
):
    head_dim, tokens = k_ref.shape[1:]
    group = q_ref.shape[0] // k_ref.shape[0]
    tiles = group * tokens // TILE
    per_tile = TILE // tokens
    span = MEMBERS * tokens

    local = [pltpu.make_async_copy(*pair, staged.at[n]) for n, pair in
             enumerate(((k_hbm, k_ref), (v_hbm, v_ref), (q_hbm, q_ref)))]
    for copy in local:
        copy.start()

    ix = lax.axis_index("cx")
    iy = lax.axis_index("cy")
    chips_x = size_x // 2
    chip_x, core = ix // 2, lax.rem(ix, 2)
    half_x, half_y = chips_x // 2, size_y // 2

    def head_of(x, y, c):
        px = lax.rem(x + x // half_x, 2)
        py = lax.rem(y + y // half_y, 2)
        return px * 4 + py * 2 + c

    def member(r):
        x = flip(chip_x) if r // 4 else chip_x
        y = flip(iy) if (r // 2) % 2 else iy
        c = flip(core) if r % 2 else core
        return {"cx": x * 2 + c, "cy": y}, head_of(x, y, c)

    my_head = head_of(chip_x, iy, core)
    mirror_x = {"cx": (chips_x - 1 - chip_x) * 2 + core, "cy": iy}
    mirror_y = {"cx": ix, "cy": size_y - 1 - iy}

    barrier = pltpu.get_barrier_semaphore()
    partners = [member(r)[0] for r in range(1, MEMBERS)] + [mirror_x, mirror_y]
    for who in partners:
        pl.semaphore_signal(barrier, inc=1, device_id=who, device_id_type=MESH)
    pl.semaphore_wait(barrier, len(partners))

    def remote(src, dst, sent, here, who):
        return pltpu.make_async_remote_copy(
            src_ref=src, dst_ref=dst, send_sem=sent, recv_sem=here, device_id=who, device_id_type=MESH
        )

    def kv_copy(kind, r):
        who, head = member(r)
        src = (k_ref, v_ref)[kind].at[head]
        return remote(src, kv_got.at[kind, 0, r], kv_sent.at[kind, r], kv_here.at[kind, r], who)

    def q_copy(r):
        who, head = member(r)
        return remote(q_ref.at[pl.ds(head * group, group)], q_got.at[r], q_sent.at[r], q_here.at[r], who)

    def forward(kind, block, r):
        index = (block - 1) * MEMBERS + r
        if block == 3:
            src, who = (kv_got.at[kind, 1, r], mirror_y) if r < 4 else (kv_got.at[kind, 2, r], mirror_x)
        else:
            src = kv_got.at[kind, 0, r] if r else (k_ref, v_ref)[kind].at[my_head]
            who = mirror_x if block == 1 else mirror_y
        return remote(src, kv_got.at[kind, block, r], fwd_sent.at[kind, index], fwd_here.at[kind, index], who)

    def out_copy(r, head):
        return remote(
            out_send.at[r], out_ref.at[pl.ds(head * group, group)], out_sent.at[r], out_here.at[r], member(r)[0]
        )

    local[KEYS].wait()
    local[VALUES].wait()
    for kind in (KEYS, VALUES):
        forward(kind, 1, 0).start()
        forward(kind, 2, 0).start()
    for some in ((1,), (4, 2, 5, 3)):
        for kind in (KEYS, VALUES):
            for r in some:
                kv_copy(kind, r).start()
    local[2].wait()
    for r in (1, 4, 2):
        q_copy(r).start()
    for kind in (KEYS, VALUES):
        for r in (6, 7):
            kv_copy(kind, r).start()
    for r in (5, 3, 6, 7):
        q_copy(r).start()

    def prepare_keys(number, slot, columns):
        base = number * span + slot * tokens
        keys[pl.ds(base, tokens)] = jnp.transpose(jnp.concatenate([columns, columns], axis=0))

    def prepare_queries(r, read):
        for g in range(group):
            wide = read(g).astype(F32) * scale
            high = wide.astype(BF16)
            rest = wide - high.astype(F32)
            middle = rest.astype(BF16)
            low = (rest - middle.astype(F32)).astype(BF16)
            cols = pl.ds(g % per_tile * tokens, tokens)
            for n, term in enumerate((high, middle, low)):
                q_limbs[r, g // per_tile, pl.ds(n * head_dim, head_dim), cols] = term

    def score(r, b):
        doubled = keys[pl.ds(b * span, span)]
        lhs = jnp.concatenate([doubled, doubled], axis=1)
        for t in range(tiles):
            s = jnp.dot(lhs, q_limbs[r, t], preferred_element_type=F32)
            scores[t] = s
            block_max[t] = jnp.max(s.reshape(span // 8, 8, TILE), axis=0)

    def step(r, b, following):
        probs, factors = [], []
        for t in range(tiles):
            old = row_max[r, t]
            new = jnp.maximum(old, jnp.max(block_max[t], axis=0, keepdims=True))
            row_max[r, t] = new
            factors.append(jnp.exp2(old - new))
            p = jnp.exp2(scores[t].reshape(span // 8, 8, TILE) - new[None])
            row_sum[r, t] = row_sum[r, t] * factors[t] + jnp.sum(p, axis=0)
            probs.append(p.reshape(span, TILE).astype(BF16))
        if following:
            score(*following)
        values = jnp.concatenate([kv_got[VALUES, block, m] for block, m in SETS[b]], axis=1)
        for t in range(tiles):
            weighted = jnp.dot(values, probs[t], preferred_element_type=F32)
            acc[r, t] = acc[r, t] * factors[t][0:1] + weighted

    def finish(r):
        for t in range(tiles):
            inverse = 1.0 / jnp.sum(row_sum[r, t], axis=0, keepdims=True)
            result = (acc[r, t] * inverse).astype(BF16)
            for n in range(per_tile):
                out_send[r, t * per_tile + n] = result[:, n * tokens:(n + 1) * tokens]

    row_max[...] = jnp.full_like(row_max, -jnp.inf)
    row_sum[...] = jnp.zeros_like(row_sum)
    acc[...] = jnp.zeros_like(acc)
    q_limbs[:, :, pl.ds(3 * head_dim, TILE - 3 * head_dim)] = jnp.zeros(
        (MEMBERS, tiles, TILE - 3 * head_dim, TILE), BF16
    )
    prepare_queries(0, lambda g: q_ref[my_head * group + g])
    prepare_keys(0, 0, k_ref[my_head])
    kv_got[VALUES, 0, 0] = v_ref[my_head]

    arrived = {(KEYS, 0, 0), (VALUES, 0, 0)}
    ready_q, ready_k = {0}, set()

    def arrive(kind, block, r):
        if (kind, block, r) in arrived:
            return
        arrived.add((kind, block, r))
        if block:
            forward(kind, block, r).wait_recv()
        else:
            kv_copy(kind, r).wait_recv()
            forward(kind, 1, r).start()
            forward(kind, 2, r).start()

    def relay(block, r):
        for kind in (KEYS, VALUES):
            arrive(kind, block, r)
            forward(kind, 3, r).start()

    def require_scores(r, b):
        if r not in ready_q:
            ready_q.add(r)
            q_copy(r).wait_recv()
            prepare_queries(r, lambda g: q_got[r, g])
        if b not in ready_k:
            ready_k.add(b)
            for block, m in SETS[b]:
                arrive(KEYS, block, m)
            for slot, (block, m) in enumerate(SETS[b]):
                if (block, m) != (0, 0):
                    prepare_keys(b, slot, kv_got[KEYS, block, m])

    def require_values(b):
        for block, m in SETS[b]:
            arrive(VALUES, block, m)

    arrive(KEYS, 0, 1)
    arrive(VALUES, 0, 1)
    require_scores(0, 0)
    order = [step for group in GROUPS for step in group]
    last = {r: n for n, (r, b) in enumerate(order)}
    score(*order[0])
    n = 0
    ended = []
    for number, members in enumerate(GROUPS):
        for following in order[n + 1:n + len(members) + 1]:
            require_scores(*following)
        for r, b in members:
            require_values(b)
        for piece in RELAYS.get(number, ()):
            relay(*piece)
        for r in ended:
            out_copy(r, my_head).start()
        ended = []
        for r, b in members:
            step(r, b, order[n + 1] if n + 1 < len(order) else None)
            if last[r] == n:
                finish(r)
                ended += [r] if r else []
            n += 1
    mine = pltpu.make_async_copy(out_send.at[0], out_ref.at[pl.ds(my_head * group, group)], out_sent.at[0])
    mine.start()

    for r in range(1, MEMBERS):
        out_copy(r, member(r)[1]).wait_recv()
        out_copy(r, my_head).wait_send()
        q_copy(r).wait_send()
    for kind in (KEYS, VALUES):
        for r in range(1, MEMBERS):
            kv_copy(kind, r).wait_send()
        for block in range(1, BLOCKS):
            for r in range(MEMBERS):
                forward(kind, block, r).wait_send()
    mine.wait()


def solution(mesh):
    size_x = mesh.shape["cx"]
    size_y = mesh.shape["cy"]
    seq_spec = P(("batch", "cx", "cy"), None, None)

    def local_attention(q_local, k_local, v_local):
        tokens, num_heads, head_dim = q_local.shape
        num_kv = k_local.shape[1]
        group = num_heads // num_kv
        tiles = group * tokens // TILE
        span = MEMBERS * tokens
        scale = 1.0 / math.sqrt(head_dim) / math.log(2.0)
        hbm = pl.BlockSpec(memory_space=pl.ANY)
        out_cols = pl.pallas_call(
            functools.partial(attend_kernel, size_x, size_y, scale),
            out_shape=jax.ShapeDtypeStruct((num_heads, head_dim, tokens), BF16),
            in_specs=[hbm] * 3,
            out_specs=hbm,
            scratch_shapes=[
                pltpu.VMEM((num_heads, head_dim, tokens), BF16),
                pltpu.VMEM((num_kv, head_dim, tokens), BF16),
                pltpu.VMEM((num_kv, head_dim, tokens), BF16),
                pltpu.VMEM((MEMBERS, group, head_dim, tokens), BF16),
                pltpu.VMEM((2, BLOCKS, MEMBERS, head_dim, tokens), BF16),
                pltpu.VMEM((BLOCKS * span, 2 * head_dim), BF16),
                pltpu.VMEM((MEMBERS, tiles, TILE, TILE), BF16),
                pltpu.VMEM((tiles, span, TILE), F32),
                pltpu.VMEM((tiles, 8, TILE), F32),
                pltpu.VMEM((MEMBERS, tiles, 8, TILE), F32),
                pltpu.VMEM((MEMBERS, tiles, 8, TILE), F32),
                pltpu.VMEM((MEMBERS, tiles, head_dim, TILE), F32),
                pltpu.VMEM((MEMBERS, group, head_dim, tokens), BF16),
                pltpu.SemaphoreType.DMA((3,)),
                pltpu.SemaphoreType.DMA((2, MEMBERS)),
                pltpu.SemaphoreType.DMA((2, MEMBERS)),
                pltpu.SemaphoreType.DMA((MEMBERS,)),
                pltpu.SemaphoreType.DMA((MEMBERS,)),
                pltpu.SemaphoreType.DMA((2, (BLOCKS - 1) * MEMBERS)),
                pltpu.SemaphoreType.DMA((2, (BLOCKS - 1) * MEMBERS)),
                pltpu.SemaphoreType.DMA((MEMBERS,)),
                pltpu.SemaphoreType.DMA((MEMBERS,)),
            ],
            compiler_params=pltpu.CompilerParams(
                collective_id=0,
                has_side_effects=True,
            ),
        )(*(jnp.transpose(x, (1, 2, 0)) for x in (q_local, k_local, v_local)))
        return jnp.transpose(out_cols, (2, 0, 1))

    return jax.shard_map(
        local_attention, mesh=mesh, in_specs=(seq_spec, seq_spec, seq_spec), out_specs=seq_spec, check_vma=False
    )
```

```python
import functools
import math

import jax
import jax.numpy as jnp
from jax import lax
from jax.experimental import pallas as pl
from jax.experimental.pallas import tpu as pltpu
from jax.sharding import PartitionSpec as P

F32 = jnp.float32
BF16 = jnp.bfloat16
MESH = pl.DeviceIdType.MESH

TILE = 256
MEMBERS = 8
BLOCKS = 4
SETS = (
    ((0, 0), (0, 1), (0, 2), (0, 3), (0, 4), (0, 5), (1, 0), (2, 0)),
    ((1, 1), (2, 1), (1, 2), (1, 3), (2, 4), (2, 5), (0, 6), (0, 7)),
    ((1, 4), (1, 5), (2, 2), (2, 3), (1, 6), (1, 7), (2, 6), (2, 7)),
    tuple((3, r) for r in range(MEMBERS)),
)
GROUPS = (
    ((0, 0),),
    ((1, 0),),
    ((4, 0),),
    ((2, 0), (4, 1), (2, 1)),
    ((5, 0), (3, 0), (5, 1), (3, 1)),
    ((6, 0), (6, 1), (6, 2)),
    ((7, 0), (7, 1), (7, 2), (5, 2)),
    ((7, 3), (6, 3), (5, 3)),
    ((3, 2), (3, 3), (4, 2), (4, 3)),
    ((2, 2), (2, 3)),
    ((1, 1), (1, 2), (1, 3)),
    ((0, 1), (0, 2), (0, 3)),
)
KEYS, VALUES = 0, 1
RELAYS = {1: ((1, 0), (1, 1)), 3: ((1, 2), (1, 3), (2, 4), (2, 5)), 5: ((2, 6), (2, 7))}


def flip(value):
    return value + 1 - 2 * lax.rem(value, 2)


def attend_kernel(
    size_x, size_y, scale,
    q_hbm, k_hbm, v_hbm, out_ref,
    q_ref, k_ref, v_ref, q_got, kv_got, keys, q_limbs, scores, block_max, row_max, row_sum, acc, out_send,
    staged, kv_sent, kv_here, q_sent, q_here, fwd_sent, fwd_here, out_sent, out_here,
):
    head_dim, tokens = k_ref.shape[1:]
    group = q_ref.shape[0] // k_ref.shape[0]
    tiles = group * tokens // TILE
    per_tile = TILE // tokens
    span = MEMBERS * tokens

    local = [pltpu.make_async_copy(*pair, staged.at[n]) for n, pair in
             enumerate(((k_hbm, k_ref), (v_hbm, v_ref), (q_hbm, q_ref)))]
    for copy in local:
        copy.start()

    ix = lax.axis_index("cx")
    iy = lax.axis_index("cy")
    chips_x = size_x // 2
    chip_x, core = ix // 2, lax.rem(ix, 2)
    half_x, half_y = chips_x // 2, size_y // 2

    def head_of(x, y, c):
        px = lax.rem(x + x // half_x, 2)
        py = lax.rem(y + y // half_y, 2)
        return px * 4 + py * 2 + c

    def member(r):
        x = flip(chip_x) if r // 4 else chip_x
        y = flip(iy) if (r // 2) % 2 else iy
        c = flip(core) if r % 2 else core
        return {"cx": x * 2 + c, "cy": y}, head_of(x, y, c)

    my_head = head_of(chip_x, iy, core)
    mirror_x = {"cx": (chips_x - 1 - chip_x) * 2 + core, "cy": iy}
    mirror_y = {"cx": ix, "cy": size_y - 1 - iy}

    barrier = pltpu.get_barrier_semaphore()
    partners = [member(r)[0] for r in range(1, MEMBERS)] + [mirror_x, mirror_y]
    for who in partners:
        pl.semaphore_signal(barrier, inc=1, device_id=who, device_id_type=MESH)
    pl.semaphore_wait(barrier, len(partners))

    def remote(src, dst, sent, here, who):
        return pltpu.make_async_remote_copy(
            src_ref=src, dst_ref=dst, send_sem=sent, recv_sem=here, device_id=who, device_id_type=MESH
        )

    def kv_copy(kind, r):
        who, head = member(r)
        src = (k_ref, v_ref)[kind].at[head]
        return remote(src, kv_got.at[kind, 0, r], kv_sent.at[kind, r], kv_here.at[kind, r], who)

    def q_copy(r):
        who, head = member(r)
        return remote(q_ref.at[pl.ds(head * group, group)], q_got.at[r], q_sent.at[r], q_here.at[r], who)

    def forward(kind, block, r):
        index = (block - 1) * MEMBERS + r
        if block == 3:
            src, who = (kv_got.at[kind, 1, r], mirror_y) if r < 4 else (kv_got.at[kind, 2, r], mirror_x)
        else:
            src = kv_got.at[kind, 0, r] if r else (k_ref, v_ref)[kind].at[my_head]
            who = mirror_x if block == 1 else mirror_y
        return remote(src, kv_got.at[kind, block, r], fwd_sent.at[kind, index], fwd_here.at[kind, index], who)

    def out_copy(r, head):
        return remote(
            out_send.at[r], out_ref.at[pl.ds(head * group, group)], out_sent.at[r], out_here.at[r], member(r)[0]
        )

    local[KEYS].wait()
    local[VALUES].wait()
    for kind in (KEYS, VALUES):
        forward(kind, 1, 0).start()
        forward(kind, 2, 0).start()
    for some in ((1,), (4, 2, 5, 3)):
        for kind in (KEYS, VALUES):
            for r in some:
                kv_copy(kind, r).start()
    local[2].wait()
    for r in (1, 4, 2):
        q_copy(r).start()
    for kind in (KEYS, VALUES):
        for r in (6, 7):
            kv_copy(kind, r).start()
    for r in (5, 3, 6, 7):
        q_copy(r).start()

    def prepare_keys(number, slot, columns):
        base = number * span + slot * tokens
        keys[pl.ds(base, tokens)] = jnp.transpose(jnp.concatenate([columns, columns], axis=0))

    def prepare_queries(r, read):
        for g in range(group):
            wide = read(g).astype(F32) * scale
            high = wide.astype(BF16)
            rest = wide - high.astype(F32)
            middle = rest.astype(BF16)
            low = (rest - middle.astype(F32)).astype(BF16)
            cols = pl.ds(g % per_tile * tokens, tokens)
            for n, term in enumerate((high, middle, low)):
                q_limbs[r, g // per_tile, pl.ds(n * head_dim, head_dim), cols] = term

    def score(r, b):
        doubled = keys[pl.ds(b * span, span)]
        lhs = jnp.concatenate([doubled, doubled], axis=1)
        for t in range(tiles):
            s = jnp.dot(lhs, q_limbs[r, t], preferred_element_type=F32)
            scores[t] = s
            block_max[t] = jnp.max(s.reshape(span // 8, 8, TILE), axis=0)

    def step(r, b, following):
        probs, factors = [], []
        for t in range(tiles):
            old = row_max[r, t]
            new = jnp.maximum(old, jnp.max(block_max[t], axis=0, keepdims=True))
            row_max[r, t] = new
            factors.append(jnp.exp2(old - new))
            p = jnp.exp2(scores[t].reshape(span // 8, 8, TILE) - new[None])
            row_sum[r, t] = row_sum[r, t] * factors[t] + jnp.sum(p, axis=0)
            probs.append(p.reshape(span, TILE).astype(BF16))
        if following:
            score(*following)
        values = jnp.concatenate([kv_got[VALUES, block, m] for block, m in SETS[b]], axis=1)
        for t in range(tiles):
            weighted = jnp.dot(values, probs[t], preferred_element_type=F32)
            acc[r, t] = acc[r, t] * factors[t][0:1] + weighted

    def finish(r):
        for t in range(tiles):
            inverse = 1.0 / jnp.sum(row_sum[r, t], axis=0, keepdims=True)
            result = (acc[r, t] * inverse).astype(BF16)
            for n in range(per_tile):
                part = result[:, n * tokens:(n + 1) * tokens]
                if r:
                    out_send[r, t * per_tile + n] = part
                else:
                    out_ref[my_head * group + t * per_tile + n] = part

    row_max[...] = jnp.full_like(row_max, -jnp.inf)
    row_sum[...] = jnp.zeros_like(row_sum)
    acc[...] = jnp.zeros_like(acc)
    q_limbs[:, :, pl.ds(3 * head_dim, TILE - 3 * head_dim)] = jnp.zeros(
        (MEMBERS, tiles, TILE - 3 * head_dim, TILE), BF16
    )
    prepare_queries(0, lambda g: q_ref[my_head * group + g])
    prepare_keys(0, 0, k_ref[my_head])
    kv_got[VALUES, 0, 0] = v_ref[my_head]

    arrived = {(KEYS, 0, 0), (VALUES, 0, 0)}
    ready_q, ready_k = {0}, set()

    def arrive(kind, block, r):
        if (kind, block, r) in arrived:
            return
        arrived.add((kind, block, r))
        if block:
            forward(kind, block, r).wait_recv()
        else:
            kv_copy(kind, r).wait_recv()
            forward(kind, 1, r).start()
            forward(kind, 2, r).start()

    def relay(block, r):
        for kind in (KEYS, VALUES):
            arrive(kind, block, r)
            forward(kind, 3, r).start()

    def require_scores(r, b):
        if r not in ready_q:
            ready_q.add(r)
            q_copy(r).wait_recv()
            prepare_queries(r, lambda g: q_got[r, g])
        if b not in ready_k:
            ready_k.add(b)
            for block, m in SETS[b]:
                arrive(KEYS, block, m)
            for slot, (block, m) in enumerate(SETS[b]):
                if (block, m) != (0, 0):
                    prepare_keys(b, slot, kv_got[KEYS, block, m])

    def require_values(b):
        for block, m in SETS[b]:
            arrive(VALUES, block, m)

    arrive(KEYS, 0, 1)
    arrive(VALUES, 0, 1)
    require_scores(0, 0)
    order = [step for group in GROUPS for step in group]
    last = {r: n for n, (r, b) in enumerate(order)}
    score(*order[0])
    n = 0
    ended = []
    for number, members in enumerate(GROUPS):
        for following in order[n + 1:n + len(members) + 1]:
            require_scores(*following)
        for r, b in members:
            require_values(b)
        for piece in RELAYS.get(number, ()):
            relay(*piece)
        for r in ended:
            out_copy(r, my_head).start()
        ended = []
        for r, b in members:
            step(r, b, order[n + 1] if n + 1 < len(order) else None)
            if last[r] == n:
                finish(r)
                ended += [r] if r else []
            n += 1
    for r in range(1, MEMBERS):
        out_copy(r, member(r)[1]).wait_recv()
        out_copy(r, my_head).wait_send()
        q_copy(r).wait_send()
    for kind in (KEYS, VALUES):
        for r in range(1, MEMBERS):
            kv_copy(kind, r).wait_send()
        for block in range(1, BLOCKS):
            for r in range(MEMBERS):
                forward(kind, block, r).wait_send()


def store_kernel(result, out_ref, stored):
    copy = pltpu.make_async_copy(result, out_ref, stored)
    copy.start()
    copy.wait()


def solution(mesh):
    size_x = mesh.shape["cx"]
    size_y = mesh.shape["cy"]
    seq_spec = P(("batch", "cx", "cy"), None, None)

    def local_attention(q_local, k_local, v_local):
        tokens, num_heads, head_dim = q_local.shape
        num_kv = k_local.shape[1]
        group = num_heads // num_kv
        tiles = group * tokens // TILE
        span = MEMBERS * tokens
        scale = 1.0 / math.sqrt(head_dim) / math.log(2.0)
        hbm = pl.BlockSpec(memory_space=pl.ANY)
        vmem = pl.BlockSpec(memory_space=pltpu.VMEM)
        out_cols = pl.pallas_call(
            functools.partial(attend_kernel, size_x, size_y, scale),
            out_shape=pltpu.VMEM((num_heads, head_dim, tokens), BF16),
            in_specs=[hbm] * 3,
            out_specs=vmem,
            scratch_shapes=[
                pltpu.VMEM((num_heads, head_dim, tokens), BF16),
                pltpu.VMEM((num_kv, head_dim, tokens), BF16),
                pltpu.VMEM((num_kv, head_dim, tokens), BF16),
                pltpu.VMEM((MEMBERS, group, head_dim, tokens), BF16),
                pltpu.VMEM((2, BLOCKS, MEMBERS, head_dim, tokens), BF16),
                pltpu.VMEM((BLOCKS * span, 2 * head_dim), BF16),
                pltpu.VMEM((MEMBERS, tiles, TILE, TILE), BF16),
                pltpu.VMEM((tiles, span, TILE), F32),
                pltpu.VMEM((tiles, 8, TILE), F32),
                pltpu.VMEM((MEMBERS, tiles, 8, TILE), F32),
                pltpu.VMEM((MEMBERS, tiles, 8, TILE), F32),
                pltpu.VMEM((MEMBERS, tiles, head_dim, TILE), F32),
                pltpu.VMEM((MEMBERS, group, head_dim, tokens), BF16),
                pltpu.SemaphoreType.DMA((3,)),
                pltpu.SemaphoreType.DMA((2, MEMBERS)),
                pltpu.SemaphoreType.DMA((2, MEMBERS)),
                pltpu.SemaphoreType.DMA((MEMBERS,)),
                pltpu.SemaphoreType.DMA((MEMBERS,)),
                pltpu.SemaphoreType.DMA((2, (BLOCKS - 1) * MEMBERS)),
                pltpu.SemaphoreType.DMA((2, (BLOCKS - 1) * MEMBERS)),
                pltpu.SemaphoreType.DMA((MEMBERS,)),
                pltpu.SemaphoreType.DMA((MEMBERS,)),
            ],
            compiler_params=pltpu.CompilerParams(
                collective_id=0,
                has_side_effects=True,
            ),
        )(*(jnp.transpose(x, (1, 2, 0)) for x in (q_local, k_local, v_local)))
        out_cols = pl.pallas_call(
            store_kernel,
            out_shape=jax.ShapeDtypeStruct(out_cols.shape, BF16),
            in_specs=[vmem],
            out_specs=hbm,
            scratch_shapes=[pltpu.SemaphoreType.DMA],
            compiler_params=pltpu.CompilerParams(vmem_limit_bytes=1024 * 1024),
        )(pltpu.with_memory_space_constraint(out_cols, pltpu.VMEM))
        return jnp.transpose(out_cols, (2, 0, 1))

    return jax.shard_map(
        local_attention, mesh=mesh, in_specs=(seq_spec, seq_spec, seq_spec), out_specs=seq_spec, check_vma=False
    )
```

```python
import functools
import math

import jax
import jax.numpy as jnp
from jax import lax
from jax.experimental import pallas as pl
from jax.experimental.pallas import tpu as pltpu
from jax.sharding import PartitionSpec as P

F32 = jnp.float32
BF16 = jnp.bfloat16
MESH = pl.DeviceIdType.MESH

TILE = 256
MEMBERS = 8
BLOCKS = 4
GROUPS = (
    ((0, 0),),
    ((1, 0),),
    ((4, 0),),
    ((2, 0),),
    ((5, 0), (3, 0)),
    ((4, 1), (2, 1), (5, 1)),
    ((3, 1), (6, 0), (7, 0), (7, 1), (6, 1)),
    ((7, 2), (6, 2), (7, 3), (6, 3)),
    ((5, 2), (5, 3), (3, 2), (3, 3)),
    ((4, 2), (4, 3), (2, 2), (2, 3)),
    ((1, 1), (1, 2), (1, 3)),
    ((0, 1), (0, 2), (0, 3)),
)
KEYS, VALUES = 0, 1
RELAYS = {3: ((KEYS, 1),), 4: ((KEYS, 2),), 5: ((VALUES, 1), (VALUES, 2))}


def flip(value):
    return value + 1 - 2 * lax.rem(value, 2)


def attend_kernel(
    size_x, size_y, scale,
    q_hbm, k_hbm, v_hbm, out_ref,
    q_ref, k_ref, v_ref, q_got, kv_got, keys, q_limbs, scores, block_max, row_max, row_sum, acc, out_send,
    staged, kv_sent, kv_here, q_sent, q_here, fwd_sent, fwd_here, out_sent, out_here,
):
    head_dim, tokens = k_ref.shape[1:]
    group = q_ref.shape[0] // k_ref.shape[0]
    tiles = group * tokens // TILE
    per_tile = TILE // tokens
    span = MEMBERS * tokens

    local = [pltpu.make_async_copy(*pair, staged.at[n]) for n, pair in
             enumerate(((k_hbm, k_ref), (v_hbm, v_ref), (q_hbm, q_ref)))]
    for copy in local:
        copy.start()

    ix = lax.axis_index("cx")
    iy = lax.axis_index("cy")
    chips_x = size_x // 2
    chip_x, core = ix // 2, lax.rem(ix, 2)
    half_x, half_y = chips_x // 2, size_y // 2

    def head_of(x, y, c):
        px = lax.rem(x + x // half_x, 2)
        py = lax.rem(y + y // half_y, 2)
        return px * 4 + py * 2 + c

    def member(r):
        x = flip(chip_x) if r // 4 else chip_x
        y = flip(iy) if (r // 2) % 2 else iy
        c = flip(core) if r % 2 else core
        return {"cx": x * 2 + c, "cy": y}, head_of(x, y, c)

    my_head = head_of(chip_x, iy, core)
    mirror_x = {"cx": (chips_x - 1 - chip_x) * 2 + core, "cy": iy}
    mirror_y = {"cx": ix, "cy": size_y - 1 - iy}

    barrier = pltpu.get_barrier_semaphore()
    partners = [member(r)[0] for r in range(1, MEMBERS)] + [mirror_x, mirror_y]
    for who in partners:
        pl.semaphore_signal(barrier, inc=1, device_id=who, device_id_type=MESH)
    pl.semaphore_wait(barrier, len(partners))

    def remote(src, dst, sent, here, who):
        return pltpu.make_async_remote_copy(
            src_ref=src, dst_ref=dst, send_sem=sent, recv_sem=here, device_id=who, device_id_type=MESH
        )

    def kv_copy(kind, r):
        who, head = member(r)
        src = (k_ref, v_ref)[kind].at[head]
        return remote(src, kv_got.at[kind, 0, r], kv_sent.at[kind, r], kv_here.at[kind, r], who)

    def q_copy(r):
        who, head = member(r)
        return remote(q_ref.at[pl.ds(head * group, group)], q_got.at[r], q_sent.at[r], q_here.at[r], who)

    def forward(kind, block, r):
        index = (block - 1) * MEMBERS + r
        if block == 3:
            src, who = (kv_got.at[kind, 1, r], mirror_y) if r < 4 else (kv_got.at[kind, 2, r], mirror_x)
        else:
            src = kv_got.at[kind, 0, r] if r else (k_ref, v_ref)[kind].at[my_head]
            who = mirror_x if block == 1 else mirror_y
        return remote(src, kv_got.at[kind, block, r], fwd_sent.at[kind, index], fwd_here.at[kind, index], who)

    def out_copy(r, head):
        return remote(
            out_send.at[r], out_ref.at[pl.ds(head * group, group)], out_sent.at[r], out_here.at[r], member(r)[0]
        )

    for kind in (KEYS, VALUES):
        local[kind].wait()
        for r in range(1, MEMBERS):
            kv_copy(kind, r).start()
        forward(kind, 1, 0).start()
        forward(kind, 2, 0).start()
    local[2].wait()
    for r in (1, 4, 2, 5, 3, 6, 7):
        q_copy(r).start()

    def prepare_keys(block, r, columns):
        base = block * span + r * tokens
        keys[pl.ds(base, tokens)] = jnp.transpose(jnp.concatenate([columns, columns], axis=0))

    def prepare_queries(r, read):
        for g in range(group):
            wide = read(g).astype(F32) * scale
            high = wide.astype(BF16)
            rest = wide - high.astype(F32)
            middle = rest.astype(BF16)
            low = (rest - middle.astype(F32)).astype(BF16)
            cols = pl.ds(g % per_tile * tokens, tokens)
            for n, term in enumerate((high, middle, low)):
                q_limbs[r, g // per_tile, pl.ds(n * head_dim, head_dim), cols] = term

    def score(r, b):
        doubled = keys[pl.ds(b * span, span)]
        lhs = jnp.concatenate([doubled, doubled], axis=1)
        for t in range(tiles):
            s = jnp.dot(lhs, q_limbs[r, t], preferred_element_type=F32)
            scores[t] = s
            block_max[t] = jnp.max(s.reshape(span // 8, 8, TILE), axis=0)

    def step(r, b, following):
        probs, factors = [], []
        for t in range(tiles):
            old = row_max[r, t]
            new = jnp.maximum(old, jnp.max(block_max[t], axis=0, keepdims=True))
            row_max[r, t] = new
            factors.append(jnp.exp2(old - new))
            p = jnp.exp2(scores[t].reshape(span // 8, 8, TILE) - new[None])
            row_sum[r, t] = row_sum[r, t] * factors[t] + jnp.sum(p, axis=0)
            probs.append(p.reshape(span, TILE).astype(BF16))
        if following:
            score(*following)
        values = jnp.concatenate([kv_got[VALUES, b, m] for m in range(MEMBERS)], axis=1)
        for t in range(tiles):
            weighted = jnp.dot(values, probs[t], preferred_element_type=F32)
            acc[r, t] = acc[r, t] * factors[t][0:1] + weighted

    def finish(r):
        for t in range(tiles):
            inverse = 1.0 / jnp.sum(row_sum[r, t], axis=0, keepdims=True)
            result = (acc[r, t] * inverse).astype(BF16)
            for n in range(per_tile):
                part = result[:, n * tokens:(n + 1) * tokens]
                if r:
                    out_send[r, t * per_tile + n] = part
                else:
                    out_ref[my_head * group + t * per_tile + n] = part

    row_max[...] = jnp.full_like(row_max, -jnp.inf)
    row_sum[...] = jnp.zeros_like(row_sum)
    acc[...] = jnp.zeros_like(acc)
    q_limbs[:, :, pl.ds(3 * head_dim, TILE - 3 * head_dim)] = jnp.zeros(
        (MEMBERS, tiles, TILE - 3 * head_dim, TILE), BF16
    )
    prepare_queries(0, lambda g: q_ref[my_head * group + g])
    prepare_keys(0, 0, k_ref[my_head])
    kv_got[VALUES, 0, 0] = v_ref[my_head]

    def values_here(m):
        kv_copy(VALUES, m).wait_recv()
        forward(VALUES, 1, m).start()
        forward(VALUES, 2, m).start()

    for some in ((1,), (2, 3, 4, 5), (6, 7)):
        for r in some:
            kv_copy(KEYS, r).wait_recv()
            forward(KEYS, 1, r).start()
            forward(KEYS, 2, r).start()
            if r == 1:
                values_here(r)
        for r in some:
            prepare_keys(0, r, kv_got[KEYS, 0, r])

    ready_q, ready_k, ready_v = {0}, {0}, set()

    def relayed(block, r):
        return (block, r // 4) in ((1, 0), (2, 1))

    def relay(kind, block):
        for m in range(MEMBERS):
            if relayed(block, m):
                forward(kind, block, m).wait_recv()
                forward(kind, 3, m).start()

    def require_scores(r, b):
        if r not in ready_q:
            ready_q.add(r)
            q_copy(r).wait_recv()
            prepare_queries(r, lambda g: q_got[r, g])
        if b not in ready_k:
            ready_k.add(b)
            for m in range(MEMBERS):
                if not relayed(b, m):
                    forward(KEYS, b, m).wait_recv()
            for m in range(MEMBERS):
                prepare_keys(b, m, kv_got[KEYS, b, m])

    def require_values(b):
        if b not in ready_v:
            ready_v.add(b)
            for m in range(MEMBERS):
                if b and not relayed(b, m):
                    forward(VALUES, b, m).wait_recv()
                if not b and m > 1:
                    values_here(m)

    order = [step for group in GROUPS for step in group]
    last = {r: n for n, (r, b) in enumerate(order)}
    score(*order[0])
    n = 0
    ended = []
    for number, members in enumerate(GROUPS):
        for kind, block in RELAYS.get(number, ()):
            relay(kind, block)
        for following in order[n + 1:n + len(members) + 1]:
            require_scores(*following)
        for r, b in members:
            require_values(b)
        for r in ended:
            out_copy(r, my_head).start()
        ended = []
        for r, b in members:
            step(r, b, order[n + 1] if n + 1 < len(order) else None)
            if last[r] == n:
                finish(r)
                ended += [r] if r else []
            n += 1
    for r in range(1, MEMBERS):
        out_copy(r, member(r)[1]).wait_recv()
        out_copy(r, my_head).wait_send()
        q_copy(r).wait_send()
    for kind in (KEYS, VALUES):
        for r in range(1, MEMBERS):
            kv_copy(kind, r).wait_send()
        for block in range(1, BLOCKS):
            for r in range(MEMBERS):
                forward(kind, block, r).wait_send()


def store_kernel(result, out_ref, stored):
    copy = pltpu.make_async_copy(result, out_ref, stored)
    copy.start()
    copy.wait()


def solution(mesh):
    size_x = mesh.shape["cx"]
    size_y = mesh.shape["cy"]
    seq_spec = P(("batch", "cx", "cy"), None, None)

    def local_attention(q_local, k_local, v_local):
        tokens, num_heads, head_dim = q_local.shape
        num_kv = k_local.shape[1]
        group = num_heads // num_kv
        tiles = group * tokens // TILE
        span = MEMBERS * tokens
        scale = 1.0 / math.sqrt(head_dim) / math.log(2.0)
        hbm = pl.BlockSpec(memory_space=pl.ANY)
        vmem = pl.BlockSpec(memory_space=pltpu.VMEM)
        out_cols = pl.pallas_call(
            functools.partial(attend_kernel, size_x, size_y, scale),
            out_shape=pltpu.VMEM((num_heads, head_dim, tokens), BF16),
            in_specs=[hbm] * 3,
            out_specs=vmem,
            scratch_shapes=[
                pltpu.VMEM((num_heads, head_dim, tokens), BF16),
                pltpu.VMEM((num_kv, head_dim, tokens), BF16),
                pltpu.VMEM((num_kv, head_dim, tokens), BF16),
                pltpu.VMEM((MEMBERS, group, head_dim, tokens), BF16),
                pltpu.VMEM((2, BLOCKS, MEMBERS, head_dim, tokens), BF16),
                pltpu.VMEM((BLOCKS * span, 2 * head_dim), BF16),
                pltpu.VMEM((MEMBERS, tiles, TILE, TILE), BF16),
                pltpu.VMEM((tiles, span, TILE), F32),
                pltpu.VMEM((tiles, 8, TILE), F32),
                pltpu.VMEM((MEMBERS, tiles, 8, TILE), F32),
                pltpu.VMEM((MEMBERS, tiles, 8, TILE), F32),
                pltpu.VMEM((MEMBERS, tiles, head_dim, TILE), F32),
                pltpu.VMEM((MEMBERS, group, head_dim, tokens), BF16),
                pltpu.SemaphoreType.DMA((3,)),
                pltpu.SemaphoreType.DMA((2, MEMBERS)),
                pltpu.SemaphoreType.DMA((2, MEMBERS)),
                pltpu.SemaphoreType.DMA((MEMBERS,)),
                pltpu.SemaphoreType.DMA((MEMBERS,)),
                pltpu.SemaphoreType.DMA((2, (BLOCKS - 1) * MEMBERS)),
                pltpu.SemaphoreType.DMA((2, (BLOCKS - 1) * MEMBERS)),
                pltpu.SemaphoreType.DMA((MEMBERS,)),
                pltpu.SemaphoreType.DMA((MEMBERS,)),
            ],
            compiler_params=pltpu.CompilerParams(
                collective_id=0,
                has_side_effects=True,
            ),
        )(*(jnp.transpose(x, (1, 2, 0)) for x in (q_local, k_local, v_local)))
        out_cols = pl.pallas_call(
            store_kernel,
            out_shape=jax.ShapeDtypeStruct(out_cols.shape, BF16),
            in_specs=[vmem],
            out_specs=hbm,
            scratch_shapes=[pltpu.SemaphoreType.DMA],
            compiler_params=pltpu.CompilerParams(vmem_limit_bytes=1024 * 1024),
        )(pltpu.with_memory_space_constraint(out_cols, pltpu.VMEM))
        return jnp.transpose(out_cols, (2, 0, 1))

    return jax.shard_map(
        local_attention, mesh=mesh, in_specs=(seq_spec, seq_spec, seq_spec), out_specs=seq_spec, check_vma=False
    )
```
